256 devices in a mesh: bank: 8 (over z_lo, y), zero: 32 (over z_hi, x, core).
Axes of the slice: x: 4, y: 4, z: 8 (z_hi: 4, z_lo: 2; z = z_hi * 2 + z_lo), core: 2. Of those that a mesh axis runs over, the one named last changes fastest.
Arguments:
- train_down: float32 [16, 6400, 4096], P('bank', None, 'zero'), may hold values from -0.15625 to 0.15625
- other_down: bfloat16 [16, 6400, 4096], P('bank', None, 'zero'), may hold values from -0.0390625 to 0.0390625
- router_weight: float32 [4096, 16], P('zero', 'bank'), may hold values from -0.09375 to 0.09375
- router_gain: float32 [4096], P('zero'), may hold values from 0.25 to 1.75
Outputs:
- ready_down: bfloat16 [16, 6400, 4096], P('bank', 'zero')
- scale_down: float32 [16, 6400], P('bank', 'zero')
- serve_router: bfloat16 [4096, 16], replicated
The draws below stay inside these ranges and needn't reach their ends.
All inputs are finite; a program needn't handle non-finite values. Where the reference program divides by a largest or mean magnitude, that divisor is 1e-20 or more.
Results may differ from the reference program's by a relative error of at most 0.001.
Values may be sent and summed in bfloat16 or wider, within the bound.
A program may use at most 64 MiB of HBM per device.

```python
import jax
import jax.numpy as jnp

EXPERTS = 16
D_MODEL = 4096
D_EXPERT = 6400


def raised(values, key, source, target, shards_of, factor):
    owner, partner = [(jnp.arange(values.shape[dim]) // (values.shape[dim] // shards_of)).reshape([-1 if axis == dim else 1 for axis in range(values.ndim)]) for dim in (source, target)]
    chosen = jax.random.permutation(key, shards_of)[partner]
    strong = (owner == chosen) | (owner == (partner + shards_of // 2) % shards_of)
    return jnp.where(strong, factor * values, values)


def level_of(key, dims, cuts, least, high):
    loudness = 1.0
    for dim, blocks in cuts:
        draws = jax.random.uniform(jax.random.fold_in(jax.random.fold_in(key, 6), dim), (blocks,), jnp.float32, least / len(cuts), high / len(cuts))
        loudness = loudness * jnp.repeat(jnp.exp(draws), dims[dim] // blocks).reshape((-1,) + (1,) * (len(dims) - 1 - dim))
    return loudness


def noise(rng, dims, deviation, reach, pieces=(), held_as=jnp.bfloat16):
    result = jax.random.normal(rng, dims, jnp.float32) * deviation
    if len(pieces) > 0:
        result = level_of(rng, dims, pieces, -0.22, 0.18) * result
    return jnp.clip(result, min=-reach, max=reach).astype(held_as)


def bell_draw_with(key, extent, scale, limit, pieces, heavy, dtype=jnp.bfloat16):
    array = scale * jax.random.normal(key, extent, jnp.float32)
    if pieces:
        array = array * level_of(key, extent, pieces, -0.22, 0.18)
    return jnp.clip(raised(array, jax.random.fold_in(key, 3), *heavy), -limit, limit).astype(dtype)


def setup_inputs(seed: int = 0) -> dict:
    streams_of = jax.random.split(jax.random.key(seed), 5)
    train_down = bell_draw_with(streams_of[0], (EXPERTS, D_EXPERT, D_MODEL), D_EXPERT ** -0.5, 0.15625, ((0, 8), (2, 32)), (2, 1, 32, 2.75), jnp.float32)
    other_down = noise(streams_of[1], (EXPERTS, D_EXPERT, D_MODEL), (D_EXPERT * 4) ** -0.5, 0.0390625, ((0, 8), (2, 32)))
    router_weight = noise(streams_of[2], (D_MODEL, EXPERTS), D_MODEL ** -0.5, 0.09375, ((0, 32), (1, 8)), jnp.float32)
    router_gain = jnp.clip(1.0 + 0.15 * jax.random.normal(streams_of[3], (D_MODEL,), jnp.float32), 0.25, 1.75)
    return {"train_down": train_down, "other_down": other_down, "router_weight": router_weight, "router_gain": router_gain}


def reference(train_down, other_down, router_weight, router_gain):
    latest_down = train_down + other_down.astype(jnp.float32)
    scale_down = jnp.max(jnp.abs(latest_down), axis=2)
    ready_down = (latest_down / jnp.expand_dims(scale_down, 2)).astype(jnp.bfloat16)
    serve_router = (router_weight * router_gain[:, None]).astype(jnp.bfloat16)
    return ready_down, scale_down, serve_router
```

```python
import functools

import jax
import jax.numpy as jnp
from jax import lax
from jax.experimental import pallas as pl
from jax.experimental.pallas import tpu as pltpu
from jax.sharding import PartitionSpec as P

MESH = pl.DeviceIdType.MESH
CHUNKS = 8
SUB, LANES = 8, 128


def remote(src, dst, send, recv, where):
    return pltpu.make_async_remote_copy(
        src_ref=src, dst_ref=dst, send_sem=send, recv_sem=recv, device_id=where, device_id_type=MESH
    )


def kernel(
    n, banks, train, other, weight, gain, ready, scale, serve,
    x_buf, o_buf, part, heard, told, inv, sent, r_in, r_out,
    in_sem, max_send, max_recv, inv_send, inv_recv, row_send, row_recv, rt_send, rt_recv, rt_own, send_sem, recv_sem, own_sem,
):
    me, bank = lax.axis_index("zero"), lax.axis_index("bank")
    experts, _, rows, _ = x_buf.shape
    tiles = rows // SUB
    per = n // CHUNKS
    lane = lax.broadcasted_iota(jnp.int32, (SUB, LANES), 1)
    row = lax.broadcasted_iota(jnp.int32, (SUB, LANES), 0)

    barrier = pltpu.get_barrier_semaphore()

    def load(g):
        at = pl.ds(g * per, per)
        return (
            pltpu.make_async_copy(train.at[:, at], x_buf.at[:, at], in_sem.at[0, g]),
            pltpu.make_async_copy(other.at[:, at], o_buf.at[:, at], in_sem.at[1, g]),
        )

    for g in range(CHUNKS):
        for copy in load(g):
            copy.start()

    @pl.loop(1, n)
    def _(k):
        pl.semaphore_signal(barrier, inc=1, device_id={"zero": lax.rem(me + k, n)}, device_id_type=MESH)

    @pl.loop(1, banks)
    def _(k):
        pl.semaphore_signal(barrier, inc=1, device_id={"bank": lax.rem(bank + k, banks)}, device_id_type=MESH)

    mine = (weight[...] * gain[...]).astype(jnp.bfloat16).astype(jnp.float32)
    r_in[bank] = mine

    @pl.loop(0, CHUNKS)
    def _(g):
        for copy in load(g):
            copy.wait()

        @pl.loop(g * per, g * per + per)
        def _(d):
            tile = jnp.zeros((SUB, LANES), jnp.float32)
            for e in range(experts):
                x = x_buf[e, d] + o_buf[e, d].astype(jnp.float32)
                x_buf[e, d] = x
                top = jnp.max(jnp.abs(x).reshape(tiles, SUB, LANES), axis=2, keepdims=True)
                for t in range(tiles):
                    tile = jnp.where(lane == e * tiles + t, top[t], tile)
            part[d] = tile

    pl.semaphore_wait(barrier, n - 1 + banks - 1)

    def to_owner(d):
        return remote(part.at[d], heard.at[me], max_send.at[d], max_recv.at[me], {"zero": d})

    @pl.loop(1, n)
    def _(k):
        to_owner(lax.rem(me + k, n)).start()

    def to_bank(b):
        return remote(r_in.at[bank], r_in.at[bank], row_send.at[b], row_recv.at[bank], {"bank": b})

    @pl.loop(1, banks)
    def _(k):
        to_bank(lax.rem(bank + k, banks)).start()

    heard[me] = part[me]

    @pl.loop(1, n)
    def _(k):
        s = lax.rem(me + k, n)
        remote(part.at[s], heard.at[s], max_send.at[s], max_recv.at[s], {"zero": s}).wait_recv()

    top = heard[0]
    for s in range(1, n):
        top = jnp.maximum(top, heard[s])
    used = lane < experts * tiles
    told[0] = jnp.where(used, 1.0 / jnp.where(used, top, 1.0), 0.0)

    for e in range(experts):
        for first in range(0, rows, LANES):
            width = min(LANES, rows - first)
            line = jnp.zeros((SUB, LANES), jnp.float32)
            for t in range(first // SUB, (first + width) // SUB):
                c = e * tiles + t
                column = jnp.broadcast_to(top[:, c : c + 1], (SUB, LANES))
                line = jnp.where(lane == t * SUB - first + row, column, line)
            scale[e : e + 1, first : first + width] = jnp.max(line, axis=0, keepdims=True)[:, :width]

    def to_all(d):
        return remote(told.at[0], inv.at[me], inv_send.at[d], inv_recv.at[me], {"zero": d})

    @pl.loop(1, n)
    def _(k):
        to_all(lax.rem(me + k, n)).start()

    inv[me] = told[0]

    def piece(d, at):
        return ready.at[:, :, pl.ds(pl.multiple_of(at * LANES, LANES), LANES)]

    def narrow(d):
        factor = inv[d]
        for e in range(experts):
            wide = [jnp.broadcast_to(factor[:, e * tiles + t : e * tiles + t + 1], (SUB, LANES)) for t in range(tiles)]
            sent[d, e] = (x_buf[e, d] * jnp.concatenate(wide, axis=0)).astype(jnp.bfloat16)

    def to_server(d):
        return remote(sent.at[d], piece(d, me), send_sem.at[d], recv_sem.at[me], {"zero": d})

    @pl.loop(1, n + 1)
    def _(k):
        @pl.when(k < n)
        def _():
            d = lax.rem(me + k, n)
            remote(told.at[0], inv.at[d], inv_send.at[d], inv_recv.at[d], {"zero": d}).wait_recv()
            narrow(d)

        @pl.when(k > 1)
        def _():
            to_server(lax.rem(me + k - 1, n)).start()

    narrow(me)

    @pl.loop(1, banks)
    def _(k):
        b = lax.rem(bank + k, banks)
        remote(r_in.at[b], r_in.at[b], row_send.at[b], row_recv.at[b], {"bank": b}).wait_recv()

    r_out[...] = jnp.concatenate([r_in[b] for b in range(banks)], axis=0).astype(jnp.bfloat16)

    own = pltpu.make_async_copy(sent.at[me], piece(me, me), own_sem)
    own.start()

    def lines(at):
        return serve.at[:, pl.ds(pl.multiple_of(at * LANES, LANES), LANES)]

    @pl.loop(1, n)
    def _(k):
        d = lax.rem(me + k, n)
        remote(r_out, lines(me), rt_send.at[d], rt_recv.at[me], {"zero": d}).start()

    kept = pltpu.make_async_copy(r_out, lines(me), rt_own)
    kept.start()

    own.wait()
    kept.wait()

    @pl.loop(1, n)
    def _(k):
        d = lax.rem(me + k, n)
        to_owner(d).wait_send()
        to_all(d).wait_send()

    @pl.loop(1, banks)
    def _(k):
        to_bank(lax.rem(bank + k, banks)).wait_send()

    @pl.loop(1, n)
    def _(k):
        d = lax.rem(me + k, n)
        remote(r_out, lines(d), rt_send.at[d], rt_recv.at[d], {"zero": d}).wait()
        remote(sent.at[d], piece(d, d), send_sem.at[d], recv_sem.at[d], {"zero": d}).wait()


def solution(mesh):
    n, banks = mesh.shape["zero"], mesh.shape["bank"]

    def local(train_down, other_down, router_weight, router_gain):
        experts, length, width = train_down.shape
        rows = length // n
        split = (experts, n, rows, width)
        dma = pltpu.SemaphoreType.DMA
        ready, scale, serve = pl.pallas_call(
            functools.partial(kernel, n, banks),
            out_shape=(
                jax.ShapeDtypeStruct((experts, rows, n * width), jnp.bfloat16),
                jax.ShapeDtypeStruct((experts, rows), jnp.float32),
                jax.ShapeDtypeStruct((banks * experts, n * width), jnp.bfloat16),
            ),
            in_specs=[pl.BlockSpec(memory_space=pltpu.HBM)] * 2 + [pl.BlockSpec(memory_space=pltpu.VMEM)] * 2,
            out_specs=(
                pl.BlockSpec(memory_space=pl.ANY),
                pl.BlockSpec(memory_space=pltpu.VMEM),
                pl.BlockSpec(memory_space=pl.ANY),
            ),
            scratch_shapes=[
                pltpu.VMEM(split, jnp.float32),
                pltpu.VMEM(split, jnp.bfloat16),
                pltpu.VMEM((n, SUB, LANES), jnp.float32),
                pltpu.VMEM((n, SUB, LANES), jnp.float32),
                pltpu.VMEM((1, SUB, LANES), jnp.float32),
                pltpu.VMEM((n, SUB, LANES), jnp.float32),
                pltpu.VMEM((n, experts, rows, width), jnp.bfloat16),
                pltpu.VMEM((banks, experts, width), jnp.float32),
                pltpu.VMEM((banks * experts, width), jnp.bfloat16),
                dma((2, CHUNKS)),
                dma((n,)), dma((n,)), dma((n,)), dma((n,)),
                dma((banks,)), dma((banks,)),
                dma((n,)), dma((n,)), dma,
                dma((n,)), dma((n,)), dma,
            ],
            compiler_params=pltpu.CompilerParams(
                collective_id=0, has_side_effects=True, vmem_limit_bytes=56 * 1024 * 1024
            ),
        )(
            train_down.reshape(split),
            other_down.reshape(split),
            router_weight.T,
            router_gain[None, :],
        )
        return ready, scale, serve.T

    in_specs = (P("bank", None, "zero"), P("bank", None, "zero"), P("zero", "bank"), P("zero"))
    out_specs = (P("bank", "zero", None), P("bank", "zero"), P())
    return jax.shard_map(local, mesh=mesh, in_specs=in_specs, out_specs=out_specs, check_vma=False)
```

```python
import functools

import jax
import jax.numpy as jnp
from jax import lax
from jax.experimental import pallas as pl
from jax.experimental.pallas import tpu as pltpu
from jax.sharding import PartitionSpec as P

MESH = pl.DeviceIdType.MESH
CHUNKS = 8
SUB, LANES = 8, 128


def remote(src, dst, send, recv, where):
    return pltpu.make_async_remote_copy(
        src_ref=src, dst_ref=dst, send_sem=send, recv_sem=recv, device_id=where, device_id_type=MESH
    )


def kernel(
    n, banks, train, other, weight, gain, ready, scale, serve,
    x_buf, o_buf, part, heard, told, inv, sent, r_in, r_out,
    in_sem, max_send, max_recv, inv_send, inv_recv, row_send, row_recv, rt_send, rt_recv, rt_own, send_sem, recv_sem, own_sem,
):
    me, bank = lax.axis_index("zero"), lax.axis_index("bank")
    experts, _, rows, _ = x_buf.shape
    tiles = rows // SUB
    per = n // CHUNKS
    lane = lax.broadcasted_iota(jnp.int32, (SUB, LANES), 1)
    row = lax.broadcasted_iota(jnp.int32, (SUB, LANES), 0)


    def peer(k):
        k = k - 1
        far = k < 24
        i = jnp.where(far, k // 3, k - 23)
        j = k % 3
        dz = jnp.where(far, jnp.where(j == 0, 1, jnp.where(j == 1, 3, 2)), 0)
        dx, dc = i // 2, i % 2
        z, x, c = (me // 8 + dz) % 4, (me // 2 + dx) % 4, (me + dc) % 2
        return z * 8 + x * 2 + c

    barrier = pltpu.get_barrier_semaphore()

    def load(g):
        at = pl.ds(g * per, per)
        return (
            pltpu.make_async_copy(train.at[:, at], x_buf.at[:, at], in_sem.at[0, g]),
            pltpu.make_async_copy(other.at[:, at], o_buf.at[:, at], in_sem.at[1, g]),
        )

    for g in range(CHUNKS):
        for copy in load(g):
            copy.start()

    @pl.loop(1, n)
    def _(k):
        pl.semaphore_signal(barrier, inc=1, device_id={"zero": peer(k)}, device_id_type=MESH)

    @pl.loop(1, banks)
    def _(k):
        pl.semaphore_signal(barrier, inc=1, device_id={"bank": lax.rem(bank + k, banks)}, device_id_type=MESH)

    mine = (weight[...] * gain[...]).astype(jnp.bfloat16).astype(jnp.float32)
    r_in[bank] = mine

    @pl.loop(0, CHUNKS)
    def _(g):
        for copy in load(g):
            copy.wait()

        @pl.loop(g * per, g * per + per)
        def _(d):
            tile = jnp.zeros((SUB, LANES), jnp.float32)
            for e in range(experts):
                x = x_buf[e, d] + o_buf[e, d].astype(jnp.float32)
                x_buf[e, d] = x
                top = jnp.max(jnp.abs(x).reshape(tiles, SUB, LANES), axis=2, keepdims=True)
                for t in range(tiles):
                    tile = jnp.where(lane == e * tiles + t, top[t], tile)
            part[d] = tile

    pl.semaphore_wait(barrier, n - 1 + banks - 1)

    def to_owner(d):
        return remote(part.at[d], heard.at[me], max_send.at[d], max_recv.at[me], {"zero": d})

    @pl.loop(1, n)
    def _(k):
        to_owner(peer(k)).start()

    def to_bank(b):
        return remote(r_in.at[bank], r_in.at[bank], row_send.at[b], row_recv.at[bank], {"bank": b})

    @pl.loop(1, banks)
    def _(k):
        to_bank(lax.rem(bank + k, banks)).start()

    heard[me] = part[me]

    @pl.loop(1, n)
    def _(k):
        s = peer(k)
        remote(part.at[s], heard.at[s], max_send.at[s], max_recv.at[s], {"zero": s}).wait_recv()

    top = heard[0]
    for s in range(1, n):
        top = jnp.maximum(top, heard[s])
    used = lane < experts * tiles
    told[0] = jnp.where(used, 1.0 / jnp.where(used, top, 1.0), 0.0)

    for e in range(experts):
        for first in range(0, rows, LANES):
            width = min(LANES, rows - first)
            line = jnp.zeros((SUB, LANES), jnp.float32)
            for t in range(first // SUB, (first + width) // SUB):
                c = e * tiles + t
                column = jnp.broadcast_to(top[:, c : c + 1], (SUB, LANES))
                line = jnp.where(lane == t * SUB - first + row, column, line)
            scale[e : e + 1, first : first + width] = jnp.max(line, axis=0, keepdims=True)[:, :width]

    def to_all(d):
        return remote(told.at[0], inv.at[me], inv_send.at[d], inv_recv.at[me], {"zero": d})

    @pl.loop(1, n)
    def _(k):
        to_all(peer(k)).start()

    inv[me] = told[0]

    def piece(d, at):
        return ready.at[:, :, pl.ds(pl.multiple_of(at * LANES, LANES), LANES)]

    def narrow(d):
        factor = inv[d]
        for e in range(experts):
            wide = [jnp.broadcast_to(factor[:, e * tiles + t : e * tiles + t + 1], (SUB, LANES)) for t in range(tiles)]
            sent[d, e] = (x_buf[e, d] * jnp.concatenate(wide, axis=0)).astype(jnp.bfloat16)

    def to_server(d):
        return remote(sent.at[d], piece(d, me), send_sem.at[d], recv_sem.at[me], {"zero": d})

    @pl.loop(1, n + 1)
    def _(k):
        @pl.when(k < n)
        def _():
            d = peer(k)
            remote(told.at[0], inv.at[d], inv_send.at[d], inv_recv.at[d], {"zero": d}).wait_recv()
            narrow(d)

        @pl.when(k > 1)
        def _():
            to_server(peer(k - 1)).start()

    narrow(me)

    @pl.loop(1, banks)
    def _(k):
        b = lax.rem(bank + k, banks)
        remote(r_in.at[b], r_in.at[b], row_send.at[b], row_recv.at[b], {"bank": b}).wait_recv()

    r_out[...] = jnp.concatenate([r_in[b] for b in range(banks)], axis=0).astype(jnp.bfloat16)

    own = pltpu.make_async_copy(sent.at[me], piece(me, me), own_sem)
    own.start()

    def lines(at):
        return serve.at[:, pl.ds(pl.multiple_of(at * LANES, LANES), LANES)]

    @pl.loop(1, n)
    def _(k):
        d = peer(k)
        remote(r_out, lines(me), rt_send.at[d], rt_recv.at[me], {"zero": d}).start()

    kept = pltpu.make_async_copy(r_out, lines(me), rt_own)
    kept.start()

    own.wait()
    kept.wait()

    @pl.loop(1, n)
    def _(k):
        d = peer(k)
        to_owner(d).wait_send()
        to_all(d).wait_send()

    @pl.loop(1, banks)
    def _(k):
        to_bank(lax.rem(bank + k, banks)).wait_send()

    @pl.loop(1, n)
    def _(k):
        d = peer(k)
        remote(r_out, lines(d), rt_send.at[d], rt_recv.at[d], {"zero": d}).wait()
        remote(sent.at[d], piece(d, d), send_sem.at[d], recv_sem.at[d], {"zero": d}).wait()


def solution(mesh):
    n, banks = mesh.shape["zero"], mesh.shape["bank"]

    def local(train_down, other_down, router_weight, router_gain):
        experts, length, width = train_down.shape
        rows = length // n
        split = (experts, n, rows, width)
        dma = pltpu.SemaphoreType.DMA
        ready, scale, serve = pl.pallas_call(
            functools.partial(kernel, n, banks),
            out_shape=(
                jax.ShapeDtypeStruct((experts, rows, n * width), jnp.bfloat16),
                jax.ShapeDtypeStruct((experts, rows), jnp.float32),
                jax.ShapeDtypeStruct((banks * experts, n * width), jnp.bfloat16),
            ),
            in_specs=[pl.BlockSpec(memory_space=pltpu.HBM)] * 2 + [pl.BlockSpec(memory_space=pltpu.VMEM)] * 2,
            out_specs=(
                pl.BlockSpec(memory_space=pl.ANY),
                pl.BlockSpec(memory_space=pltpu.VMEM),
                pl.BlockSpec(memory_space=pl.ANY),
            ),
            scratch_shapes=[
                pltpu.VMEM(split, jnp.float32),
                pltpu.VMEM(split, jnp.bfloat16),
                pltpu.VMEM((n, SUB, LANES), jnp.float32),
                pltpu.VMEM((n, SUB, LANES), jnp.float32),
                pltpu.VMEM((1, SUB, LANES), jnp.float32),
                pltpu.VMEM((n, SUB, LANES), jnp.float32),
                pltpu.VMEM((n, experts, rows, width), jnp.bfloat16),
                pltpu.VMEM((banks, experts, width), jnp.float32),
                pltpu.VMEM((banks * experts, width), jnp.bfloat16),
                dma((2, CHUNKS)),
                dma((n,)), dma((n,)), dma((n,)), dma((n,)),
                dma((banks,)), dma((banks,)),
                dma((n,)), dma((n,)), dma,
                dma((n,)), dma((n,)), dma,
            ],
            compiler_params=pltpu.CompilerParams(
                collective_id=0, has_side_effects=True, vmem_limit_bytes=48 * 1024 * 1024
            ),
        )(
            train_down.reshape(split),
            other_down.reshape(split),
            router_weight.T,
            router_gain[None, :],
        )
        return ready, scale, serve.T

    in_specs = (P("bank", None, "zero"), P("bank", None, "zero"), P("zero", "bank"), P("zero"))
    out_specs = (P("bank", "zero", None), P("bank", "zero"), P())
    return jax.shard_map(local, mesh=mesh, in_specs=in_specs, out_specs=out_specs, check_vma=False)
```

```python
import functools

import jax
import jax.numpy as jnp
from jax import lax
from jax.experimental import pallas as pl
from jax.experimental.pallas import tpu as pltpu
from jax.sharding import PartitionSpec as P

MESH = pl.DeviceIdType.MESH
SUB, LANES = 8, 128
HALF = SUB // 2
PLANES = 4
CHUNKS = 8
UNIT = 40
SLABS = 2
EARLY, PACE = 6, 1
DURING = 6


def remote(src, dst, send, recv, where):
    return pltpu.make_async_remote_copy(
        src_ref=src, dst_ref=dst, send_sem=send, recv_sem=recv, device_id=where, device_id_type=MESH
    )


def kernel(
    n, banks, train, other, weight, gain, ready, scale, serve,
    x_buf, o_buf, w_buf, g_buf, loose, part, heard, told, inv, sent, lines, raw_in,
    in_sem, max_send, max_recv, inv_send, inv_recv, row_send, row_recv, line_send, line_recv,
    send_sem, recv_sem, own_sem, raw_send, raw_recv,
):
    me, bank = lax.axis_index("zero"), lax.axis_index("bank")
    experts, _, rows, _ = x_buf.shape
    tiles, units = rows // SUB, rows // UNIT
    per, plane = n // CHUNKS, n // PLANES
    lane = lax.broadcasted_iota(jnp.int32, (SUB, LANES), 1)
    row = lax.broadcasted_iota(jnp.int32, (SUB, LANES), 0)

    def peer(up, i):
        z, x, c = lax.rem(me // plane + up, PLANES), lax.rem(me % plane // 2 + i // 2, plane // 2), lax.rem(me + i, 2)
        return z * plane + x * 2 + c

    def back(up, i):
        z, x, c = lax.rem(me // plane + PLANES - up, PLANES), lax.rem(me % plane // 2 + plane // 2 - i // 2, plane // 2), lax.rem(me + i, 2)
        return z * plane + x * 2 + c

    half = lax.broadcasted_iota(jnp.int32, (HALF, LANES), 1)

    def packed(tile):
        return jnp.where(half < LANES // 2, tile[:HALF], pltpu.roll(tile[HALF:], LANES // 2, 1))

    def spread(tile):
        return jnp.concatenate([tile, pltpu.roll(tile, LANES // 2, 1)], axis=0)

    def others(body, ups=(2, 1, 3, 0)):
        for up in ups:

            @pl.loop(1 if up == 0 else 0, plane)
            def _(i):
                body(peer(up, i))

    def chunk(k):
        return lax.rem(me // per + plane // per + k, CHUNKS)

    def load(k):
        g = chunk(k)
        at = pl.ds(g * per, per)
        return (
            pltpu.make_async_copy(train.at[:, at], x_buf.at[:, at], in_sem.at[0, g]),
            pltpu.make_async_copy(other.at[:, at], o_buf.at[:, at], in_sem.at[1, g]),
        )

    small = (
        pltpu.make_async_copy(weight, w_buf, in_sem.at[0, CHUNKS]),
        pltpu.make_async_copy(gain, g_buf, in_sem.at[1, CHUNKS]),
    )
    barrier = pltpu.get_barrier_semaphore()
    for k in range(CHUNKS):
        for copy in load(k):
            copy.start()
    others(lambda d: pl.semaphore_signal(barrier, inc=1, device_id={"zero": d}, device_id_type=MESH))
    for copy in small:
        copy.start()

    across = lax.rem(bank + banks // 2, banks)
    row_of = banks // 2
    beside = [bank // row_of * row_of + lax.rem(bank + k, row_of) for k in range(1, row_of)]
    for b in [across] + beside:
        pl.semaphore_signal(barrier, inc=1, device_id={"bank": b}, device_id_type=MESH)

    def raw(way, u):
        slab, unit = u // units, u % units
        e, i = slab % experts, slab // experts
        d, at = peer(1 + 2 * way, i), pl.ds(unit * UNIT, UNIT)
        return remote(x_buf.at[e, d, at], raw_in.at[way, slab, at], raw_send.at[way, u], raw_recv.at[way, u], {"zero": d})

    def raws(first, last):
        for u in range(first, last):
            for way in range(2):
                raw(way, u).start()

    def maxima(k):
        for copy in load(k):
            copy.wait()
        for j in range(per):
            d = chunk(k) * per + j
            tile = jnp.zeros((SUB, LANES), jnp.float32)
            for e in range(experts):
                x = x_buf[e, d] + o_buf[e, d].astype(jnp.float32)
                x_buf[e, d] = x
                top = jnp.max(jnp.abs(x).reshape(tiles, SUB, LANES), axis=2, keepdims=True)
                for t in range(tiles):
                    tile = jnp.where(lane == e * tiles + t, top[t], tile)
            loose[d] = tile

    pl.loop(0, EARLY)(maxima)
    pl.semaphore_wait(barrier, n - 1 + row_of)

    @pl.loop(EARLY, CHUNKS)
    def _(g):
        maxima(g)
        for way in range(2):
            for k in range(PACE):
                raw(way, (g - EARLY) * PACE + k).start()

    for d in range(n):
        part[d] = packed(loose[d])

    def to_owner(d):
        return remote(part.at[d], heard.at[me], max_send.at[d], max_recv.at[me], {"zero": d})

    others(lambda d: to_owner(d).start())

    raws((CHUNKS - EARLY) * PACE, (CHUNKS - EARLY) * PACE + DURING)

    for copy in small:
        copy.wait()
    lines[bank, me] = (w_buf[...] * g_buf[...]).astype(jnp.bfloat16).astype(jnp.float32)

    def to_rows(d):
        return remote(lines.at[bank, me], lines.at[bank, me], row_send.at[d], row_recv.at[me], {"zero": d})

    def from_rows(s):
        remote(lines.at[bank, s], lines.at[bank, s], row_send.at[s], row_recv.at[s], {"zero": s}).wait_recv()

    def line(at, to, k):
        return remote(lines.at[at], lines.at[at], line_send.at[k], line_recv.at[k], {"bank": to})

    others(lambda d: to_rows(d).start())

    heard[me] = part[me]

    @pl.loop(0, n)
    def _(s):
        @pl.when(s != me)
        def _():
            remote(part.at[s], heard.at[s], max_send.at[s], max_recv.at[s], {"zero": s}).wait_recv()

    top = heard[0]
    for s in range(1, n):
        top = jnp.maximum(top, heard[s])
    used = lax.rem(half, LANES // 2) < experts * tiles
    told[0] = jnp.where(used, 1.0 / jnp.where(used, top, 1.0), 0.0)
    top = spread(top)

    def to_all(d):
        return remote(told.at[0], inv.at[me], inv_send.at[d], inv_recv.at[me], {"zero": d})

    others(lambda d: to_all(d).start(), (1, 3, 2, 0))

    raws((CHUNKS - EARLY) * PACE + DURING, SLABS * units)

    def piece(e, at):
        return ready.at[e, :, pl.ds(pl.multiple_of(at * LANES, LANES), LANES)]

    def narrow(d, e, source, factor):
        factor = spread(factor)
        wide = [jnp.broadcast_to(factor[:, e * tiles + t : e * tiles + t + 1], (SUB, LANES)) for t in range(tiles)]
        sent[d, e] = (source * jnp.concatenate(wide, axis=0)).astype(jnp.bfloat16)

    def to_server(d, e):
        return remote(sent.at[d, e], piece(e, me), send_sem.at[d, e], recv_sem.at[me, e], {"zero": d})

    def known(d):
        remote(told.at[0], inv.at[d], inv_send.at[d], inv_recv.at[d], {"zero": d}).wait_recv()

    def step(up, i, was):
        d = peer(up, i)
        known(d)
        for e in range(experts):
            narrow(d, e, x_buf[e, d], inv[d])
        for e in range(experts):
            to_server(was, e).start()
        return d

    halves = [(peer(up, slab // experts), slab % experts) for slab in range(SLABS, -(-SLABS // experts) * experts) for up in (1, 3)]
    whole = -(-SLABS // experts)
    for up in (1, 3):
        for i in range(whole):
            known(peer(up, i))
    for d, e in halves:
        narrow(d, e, x_buf[e, d], inv[d])
    was = peer(1, whole)
    known(was)
    for e in range(experts):
        narrow(was, e, x_buf[e, was], inv[was])
    for d, e in halves:
        to_server(d, e).start()
    was = step(3, whole, was)

    @pl.loop(0, n)
    def _(s):
        @pl.when(s != me)
        def _():
            from_rows(s)

    line(bank, across, 0).start()

    was = lax.fori_loop(whole + 1, 4, lambda i, was: step(3, i, step(1, i, was)), was)

    line(bank, across, 0).wait()
    for k, b in enumerate(beside):
        line(bank, b, 1 + k).start()
        line(across, b, row_of + k).start()

    was = lax.fori_loop(0, 4, lambda i, was: step(2, i, was), was)
    was = lax.fori_loop(4, plane, lambda i, was: step(2, i, step(3, i, step(1, i, was))), was)
    was = lax.fori_loop(1, plane, lambda i, was: step(0, i, was), was)
    for e in range(experts):
        to_server(was, e).start()

    for e in range(experts):
        narrow(me, e, x_buf[e, me], told[0])
    local = [pltpu.make_async_copy(sent.at[me, e], piece(e, me), own_sem.at[e]) for e in range(experts)]
    for copy in local:
        copy.start()
    for slab in range(SLABS):
        e, i = slab % experts, slab // experts
        for way in range(2):
            slot, source = peer(1 + 2 * way, i), back(1 + 2 * way, i)
            for u in range(slab * units, slab * units + units):
                raw(way, u).wait()
            narrow(slot, e, raw_in[way, slab], told[0])
            local.append(pltpu.make_async_copy(sent.at[slot, e], piece(e, source), own_sem.at[experts + 2 * slab + way]))
            local[-1].start()

    for e in range(experts):
        for first in range(0, rows, LANES):
            width = min(LANES, rows - first)
            strip = jnp.zeros((SUB, LANES), jnp.float32)
            for t in range(first // SUB, (first + width) // SUB):
                c = e * tiles + t
                column = jnp.broadcast_to(top[:, c : c + 1], (SUB, LANES))
                strip = jnp.where(lane == t * SUB - first + row, column, strip)
            scale[e : e + 1, first : first + width] = jnp.max(strip, axis=0, keepdims=True)[:, :width]

    for copy in local:
        copy.wait()
    for k in range(1, row_of):
        b = bank // row_of * row_of + lax.rem(bank + row_of - k, row_of)
        far = lax.rem(b + banks // 2, banks)
        line(bank, beside[k - 1], k).wait_send()
        line(across, beside[k - 1], row_of + k - 1).wait_send()
        remote(lines.at[b], lines.at[b], line_send.at[k], line_recv.at[k], {"bank": b}).wait_recv()
        remote(lines.at[far], lines.at[far], line_send.at[row_of + k - 1], line_recv.at[row_of + k - 1], {"bank": b}).wait_recv()
    for s in range(n):
        columns = jnp.concatenate([lines[b, s] for b in range(banks)], axis=0)
        serve[:, s * LANES : (s + 1) * LANES] = columns.astype(jnp.bfloat16)

    gone = [peer(up, i) for i in range(whole) for up in (1, 3)]
    came = [back(up, i) for i in range(whole) for up in (1, 3)]

    @pl.loop(0, n)
    def _(d):
        @pl.when(d != me)
        def _():
            to_owner(d).wait_send()
            to_all(d).wait_send()
            to_rows(d).wait_send()

        for those, done in ((gone, "wait_send"), (came, "wait_recv")):
            here = d != me
            for it in those:
                here = jnp.logical_and(here, d != it)

            @pl.when(here)
            def _():
                for e in range(experts):
                    getattr(remote(sent.at[d, e], piece(e, d), send_sem.at[d, e], recv_sem.at[d, e], {"zero": d}), done)()

    for d, e in halves:
        to_server(d, e).wait_send()
    for slab in range(SLABS, whole * experts):
        for up in (1, 3):
            s, e = back(up, slab // experts), slab % experts
            remote(sent.at[s, e], piece(e, s), send_sem.at[s, e], recv_sem.at[s, e], {"zero": s}).wait_recv()


def deliver(ready, scale, serve, ready_out, scale_out, serve_out, sem):
    experts = ready.shape[0]
    copies = [pltpu.make_async_copy(ready.at[e], ready_out.at[e], sem.at[e]) for e in range(experts)]
    copies.append(pltpu.make_async_copy(scale, scale_out, sem.at[experts]))
    copies.append(pltpu.make_async_copy(serve, serve_out, sem.at[experts + 1]))
    for copy in copies:
        copy.start()
    for copy in copies:
        copy.wait()


def solution(mesh):
    n, banks = mesh.shape["zero"], mesh.shape["bank"]

    def local(train_down, other_down, router_weight, router_gain):
        experts, length, width = train_down.shape
        rows = length // n
        split = (experts, n, rows, width)
        dma, vmem = pltpu.SemaphoreType.DMA, pltpu.VMEM
        units = SLABS * rows // UNIT
        outs = (
            jax.ShapeDtypeStruct((experts, rows, n * width), jnp.bfloat16),
            jax.ShapeDtypeStruct((experts, rows), jnp.float32),
            jax.ShapeDtypeStruct((banks * experts, n * width), jnp.bfloat16),
        )
        anywhere = pl.BlockSpec(memory_space=pl.ANY)
        inputs = (train_down.reshape(split), other_down.reshape(split), router_weight.T, router_gain[None, :])
        results = pl.pallas_call(
            functools.partial(kernel, n, banks),
            out_shape=outs,
            in_specs=[pl.BlockSpec(memory_space=pltpu.HBM)] * 4,
            out_specs=(anywhere,) + (pl.BlockSpec(memory_space=vmem),) * 2,
            scratch_shapes=[
                vmem(split, jnp.float32),
                vmem(split, jnp.bfloat16),
                vmem((experts, width), jnp.float32),
                vmem((1, width), jnp.float32),
                vmem((n, SUB, LANES), jnp.float32),
                vmem((n, HALF, LANES), jnp.float32),
                vmem((n, HALF, LANES), jnp.float32),
                vmem((1, HALF, LANES), jnp.float32),
                vmem((n, HALF, LANES), jnp.float32),
                vmem((n, experts, rows, width), jnp.bfloat16),
                vmem((banks, n, experts, width), jnp.float32),
                vmem((2, SLABS, rows, width), jnp.float32),
                dma((2, CHUNKS + 1)),
                dma((n,)), dma((n,)), dma((n,)), dma((n,)),
                dma((n,)), dma((n,)), dma((banks,)), dma((banks,)),
                dma((n, experts)), dma((n, experts)), dma((experts + 2 * SLABS,)),
                dma((2, units)), dma((2, units)),
            ],
            compiler_params=pltpu.CompilerParams(
                collective_id=0, has_side_effects=True, vmem_limit_bytes=40 * 1024 * 1024
            ),
        )(*(pltpu.with_memory_space_constraint(a, pltpu.HBM) for a in inputs))
        ready, scale, serve = pl.pallas_call(
            deliver,
            out_shape=outs,
            in_specs=[anywhere] * 3,
            out_specs=(anywhere,) * 3,
            scratch_shapes=[dma((experts + 2,))],
            compiler_params=pltpu.CompilerParams(vmem_limit_bytes=1024 * 1024),
        )(*results)
        return ready, scale, serve.T

    in_specs = (P("bank", None, "zero"), P("bank", None, "zero"), P("zero", "bank"), P("zero"))
    out_specs = (P("bank", "zero"), P("bank", "zero"), P())
    return jax.shard_map(local, mesh=mesh, in_specs=in_specs, out_specs=out_specs, check_vma=False)
```

```python
import functools

import jax
import jax.numpy as jnp
from jax import lax
from jax.experimental import pallas as pl
from jax.experimental.pallas import tpu as pltpu
from jax.sharding import PartitionSpec as P

MESH = pl.DeviceIdType.MESH
SUB, LANES = 8, 128
HALF = SUB // 2
PLANES = 4
CHUNKS = 8
UNIT = 40
SLABS = 2
EARLY, PACE = 6, 1
DURING = 6


def remote(src, dst, send, recv, where):
    return pltpu.make_async_remote_copy(
        src_ref=src, dst_ref=dst, send_sem=send, recv_sem=recv, device_id=where, device_id_type=MESH
    )


def kernel(
    n, banks, train, other, weight, gain, ready, scale, serve,
    x_buf, o_buf, w_buf, g_buf, loose, part, heard, told, inv, sent, lines, raw_in,
    in_sem, max_send, max_recv, inv_send, inv_recv, row_send, row_recv, line_send, line_recv,
    send_sem, recv_sem, own_sem, raw_send, raw_recv,
):
    me, bank = lax.axis_index("zero"), lax.axis_index("bank")
    experts, _, rows, _ = x_buf.shape
    tiles, units = rows // SUB, rows // UNIT
    per, plane = n // CHUNKS, n // PLANES
    lane = lax.broadcasted_iota(jnp.int32, (SUB, LANES), 1)
    row = lax.broadcasted_iota(jnp.int32, (SUB, LANES), 0)

    def peer(up, i):
        z, x, c = lax.rem(me // plane + up, PLANES), lax.rem(me % plane // 2 + i // 2, plane // 2), lax.rem(me + i, 2)
        return z * plane + x * 2 + c

    def back(up, i):
        z, x, c = lax.rem(me // plane + PLANES - up, PLANES), lax.rem(me % plane // 2 + plane // 2 - i // 2, plane // 2), lax.rem(me + i, 2)
        return z * plane + x * 2 + c

    half = lax.broadcasted_iota(jnp.int32, (HALF, LANES), 1)

    def packed(tile):
        return jnp.where(half < LANES // 2, tile[:HALF], pltpu.roll(tile[HALF:], LANES // 2, 1))

    def spread(tile):
        return jnp.concatenate([tile, pltpu.roll(tile, LANES // 2, 1)], axis=0)

    def others(body, ups=(2, 1, 3, 0)):
        for up in ups:

            @pl.loop(1 if up == 0 else 0, plane)
            def _(i):
                body(peer(up, i))

    def chunk(k):
        return lax.rem(me // per + plane // per + k, CHUNKS)

    def load(k):
        g = chunk(k)
        at = pl.ds(g * per, per)
        return (
            pltpu.make_async_copy(train.at[:, at], x_buf.at[:, at], in_sem.at[0, g]),
            pltpu.make_async_copy(other.at[:, at], o_buf.at[:, at], in_sem.at[1, g]),
        )

    small = (
        pltpu.make_async_copy(weight, w_buf, in_sem.at[0, CHUNKS]),
        pltpu.make_async_copy(gain, g_buf, in_sem.at[1, CHUNKS]),
    )
    barrier = pltpu.get_barrier_semaphore()
    for k in range(CHUNKS):
        for copy in load(k):
            copy.start()
    others(lambda d: pl.semaphore_signal(barrier, inc=1, device_id={"zero": d}, device_id_type=MESH))
    for copy in small:
        copy.start()

    across = lax.rem(bank + banks // 2, banks)
    row_of = banks // 2
    beside = [bank // row_of * row_of + lax.rem(bank + k, row_of) for k in range(1, row_of)]
    for b in [across] + beside:
        pl.semaphore_signal(barrier, inc=1, device_id={"bank": b}, device_id_type=MESH)

    def raw(way, u):
        slab, unit = u // units, u % units
        e, i = slab % experts, slab // experts
        d, at = peer(1 + 2 * way, i), pl.ds(unit * UNIT, UNIT)
        return remote(x_buf.at[e, d, at], raw_in.at[way, slab, at], raw_send.at[way, u], raw_recv.at[way, u], {"zero": d})

    def raws(first, last):
        for u in range(first, last):
            for way in range(2):
                raw(way, u).start()

    def maxima(k):
        for copy in load(k):
            copy.wait()
        for j in range(per):
            d = chunk(k) * per + j
            tile = jnp.zeros((SUB, LANES), jnp.float32)
            for e in range(experts):
                x = x_buf[e, d] + o_buf[e, d].astype(jnp.float32)
                x_buf[e, d] = x
                top = jnp.max(jnp.abs(x).reshape(tiles, SUB, LANES), axis=2, keepdims=True)
                for t in range(tiles):
                    tile = jnp.where(lane == e * tiles + t, top[t], tile)
            loose[d] = tile

    pl.loop(0, EARLY)(maxima)
    pl.semaphore_wait(barrier, n - 1 + row_of)

    @pl.loop(EARLY, CHUNKS)
    def _(g):
        maxima(g)
        for way in range(2):
            for k in range(PACE):
                raw(way, (g - EARLY) * PACE + k).start()

    for d in range(n):
        part[d] = packed(loose[d])

    def to_owner(d):
        return remote(part.at[d], heard.at[me], max_send.at[d], max_recv.at[me], {"zero": d})

    others(lambda d: to_owner(d).start())

    raws((CHUNKS - EARLY) * PACE, (CHUNKS - EARLY) * PACE + DURING)

    for copy in small:
        copy.wait()
    lines[bank, me] = (w_buf[...] * g_buf[...]).astype(jnp.bfloat16)

    def to_rows(d):
        return remote(lines.at[bank, me], lines.at[bank, me], row_send.at[d], row_recv.at[me], {"zero": d})

    def from_rows(s):
        remote(lines.at[bank, s], lines.at[bank, s], row_send.at[s], row_recv.at[s], {"zero": s}).wait_recv()

    def line(at, to, k):
        return remote(lines.at[at], lines.at[at], line_send.at[k], line_recv.at[k], {"bank": to})

    others(lambda d: to_rows(d).start())

    heard[me] = part[me]

    @pl.loop(0, n)
    def _(s):
        @pl.when(s != me)
        def _():
            remote(part.at[s], heard.at[s], max_send.at[s], max_recv.at[s], {"zero": s}).wait_recv()

    top = heard[0]
    for s in range(1, n):
        top = jnp.maximum(top, heard[s])
    used = lax.rem(half, LANES // 2) < experts * tiles
    told[0] = jnp.where(used, 1.0 / jnp.where(used, top, 1.0), 0.0)
    top = spread(top)

    def to_all(d):
        return remote(told.at[0], inv.at[me], inv_send.at[d], inv_recv.at[me], {"zero": d})

    others(lambda d: to_all(d).start(), (1, 3, 2, 0))

    raws((CHUNKS - EARLY) * PACE + DURING, SLABS * units)

    def piece(e, at):
        return ready.at[e, :, pl.ds(pl.multiple_of(at * LANES, LANES), LANES)]

    def narrow(d, e, source, factor):
        factor = spread(factor)
        wide = [jnp.broadcast_to(factor[:, e * tiles + t : e * tiles + t + 1], (SUB, LANES)) for t in range(tiles)]
        sent[d, e] = (source * jnp.concatenate(wide, axis=0)).astype(jnp.bfloat16)

    def to_server(d, e):
        return remote(sent.at[d, e], piece(e, me), send_sem.at[d, e], recv_sem.at[me, e], {"zero": d})

    def known(d):
        remote(told.at[0], inv.at[d], inv_send.at[d], inv_recv.at[d], {"zero": d}).wait_recv()

    def step(up, i, was):
        d = peer(up, i)
        known(d)
        for e in range(experts):
            narrow(d, e, x_buf[e, d], inv[d])
        for e in range(experts):
            to_server(was, e).start()
        return d

    halves = [(peer(up, slab // experts), slab % experts) for slab in range(SLABS, -(-SLABS // experts) * experts) for up in (1, 3)]
    whole = -(-SLABS // experts)
    for d, e in halves:
        known(d)
        narrow(d, e, x_buf[e, d], inv[d])
    was = peer(1, whole)
    known(was)
    for e in range(experts):
        narrow(was, e, x_buf[e, was], inv[was])
    for d, e in halves:
        to_server(d, e).start()
    was = step(3, whole, was)

    @pl.loop(0, n)
    def _(s):
        @pl.when(s != me)
        def _():
            from_rows(s)

    line(bank, across, 0).start()

    was = lax.fori_loop(whole + 1, 4, lambda i, was: step(3, i, step(1, i, was)), was)

    was = lax.fori_loop(0, 4, lambda i, was: step(2, i, was), was)
    was = lax.fori_loop(4, plane, lambda i, was: step(2, i, step(3, i, step(1, i, was))), was)

    line(bank, across, 0).wait()
    for k, b in enumerate(beside):
        line(bank, b, 1 + k).start()
        line(across, b, row_of + k).start()

    was = lax.fori_loop(1, plane, lambda i, was: step(0, i, was), was)
    for e in range(experts):
        to_server(was, e).start()

    for e in range(experts):
        narrow(me, e, x_buf[e, me], told[0])
    local = [pltpu.make_async_copy(sent.at[me, e], piece(e, me), own_sem.at[e]) for e in range(experts)]
    for copy in local:
        copy.start()
    for slab in range(SLABS):
        e, i = slab % experts, slab // experts
        for way in range(2):
            slot, source = peer(1 + 2 * way, i), back(1 + 2 * way, i)
            for u in range(slab * units, slab * units + units):
                raw(way, u).wait()
            narrow(slot, e, raw_in[way, slab], told[0])
            local.append(pltpu.make_async_copy(sent.at[slot, e], piece(e, source), own_sem.at[experts + 2 * slab + way]))
            local[-1].start()

    for e in range(experts):
        for first in range(0, rows, LANES):
            width = min(LANES, rows - first)
            strip = jnp.zeros((SUB, LANES), jnp.float32)
            for t in range(first // SUB, (first + width) // SUB):
                c = e * tiles + t
                column = jnp.broadcast_to(top[:, c : c + 1], (SUB, LANES))
                strip = jnp.where(lane == t * SUB - first + row, column, strip)
            scale[e : e + 1, first : first + width] = jnp.max(strip, axis=0, keepdims=True)[:, :width]

    for copy in local:
        copy.wait()
    for k in range(1, row_of):
        b = bank // row_of * row_of + lax.rem(bank + row_of - k, row_of)
        far = lax.rem(b + banks // 2, banks)
        line(bank, beside[k - 1], k).wait_send()
        line(across, beside[k - 1], row_of + k - 1).wait_send()
        remote(lines.at[b], lines.at[b], line_send.at[k], line_recv.at[k], {"bank": b}).wait_recv()
        remote(lines.at[far], lines.at[far], line_send.at[row_of + k - 1], line_recv.at[row_of + k - 1], {"bank": b}).wait_recv()
    for s in range(n):
        columns = jnp.concatenate([lines[b, s].astype(jnp.float32) for b in range(banks)], axis=0)
        serve[:, s * LANES : (s + 1) * LANES] = columns.astype(jnp.bfloat16)

    @pl.loop(0, n)
    def _(d):
        @pl.when(d != me)
        def _():
            to_owner(d).wait_send()
            to_all(d).wait_send()
            to_rows(d).wait_send()

    for i in range(SLABS // experts):
        for up in (1, 3):
            known(peer(up, i))

    for slab in range(SLABS, whole * experts):
        for up in (1, 3):
            d, s, e = peer(up, slab // experts), back(up, slab // experts), slab % experts
            to_server(d, e).wait_send()
            remote(sent.at[s, e], piece(e, s), send_sem.at[s, e], recv_sem.at[s, e], {"zero": s}).wait_recv()

    def over(up, i):
        d, s = peer(up, i), back(up, i)
        for e in range(experts):
            to_server(d, e).wait_send()
            remote(sent.at[s, e], piece(e, s), send_sem.at[s, e], recv_sem.at[s, e], {"zero": s}).wait_recv()

    for lo, hi, ups in ((whole, 4, (1, 3)), (0, 4, (2,)), (4, plane, (1, 3, 2)), (1, plane, (0,))):

        @pl.loop(lo, hi)
        def _(i):
            for up in ups:
                over(up, i)


def deliver(ready, scale, serve, ready_out, scale_out, serve_out, sem):
    experts = ready.shape[0]
    copies = [pltpu.make_async_copy(ready.at[e], ready_out.at[e], sem.at[e]) for e in range(experts)]
    copies.append(pltpu.make_async_copy(scale, scale_out, sem.at[experts]))
    copies.append(pltpu.make_async_copy(serve, serve_out, sem.at[experts + 1]))
    for copy in copies:
        copy.start()
    for copy in copies:
        copy.wait()


def solution(mesh):
    n, banks = mesh.shape["zero"], mesh.shape["bank"]

    def local(train_down, other_down, router_weight, router_gain):
        experts, length, width = train_down.shape
        rows = length // n
        split = (experts, n, rows, width)
        dma, vmem = pltpu.SemaphoreType.DMA, pltpu.VMEM
        units = SLABS * rows // UNIT
        outs = (
            jax.ShapeDtypeStruct((experts, rows, n * width), jnp.bfloat16),
            jax.ShapeDtypeStruct((experts, rows), jnp.float32),
            jax.ShapeDtypeStruct((banks * experts, n * width), jnp.bfloat16),
        )
        anywhere = pl.BlockSpec(memory_space=pl.ANY)
        inputs = (train_down.reshape(split), other_down.reshape(split), router_weight.T, router_gain[None, :])
        results = pl.pallas_call(
            functools.partial(kernel, n, banks),
            out_shape=outs,
            in_specs=[pl.BlockSpec(memory_space=pltpu.HBM)] * 4,
            out_specs=(anywhere,) + (pl.BlockSpec(memory_space=vmem),) * 2,
            scratch_shapes=[
                vmem(split, jnp.float32),
                vmem(split, jnp.bfloat16),
                vmem((experts, width), jnp.float32),
                vmem((1, width), jnp.float32),
                vmem((n, SUB, LANES), jnp.float32),
                vmem((n, HALF, LANES), jnp.float32),
                vmem((n, HALF, LANES), jnp.float32),
                vmem((1, HALF, LANES), jnp.float32),
                vmem((n, HALF, LANES), jnp.float32),
                vmem((n, experts, rows, width), jnp.bfloat16),
                vmem((banks, n, experts, width), jnp.bfloat16),
                vmem((2, SLABS, rows, width), jnp.float32),
                dma((2, CHUNKS + 1)),
                dma((n,)), dma((n,)), dma((n,)), dma((n,)),
                dma((n,)), dma((n,)), dma((banks,)), dma((banks,)),
                dma((n, experts)), dma((n, experts)), dma((experts + 2 * SLABS,)),
                dma((2, units)), dma((2, units)),
            ],
            compiler_params=pltpu.CompilerParams(
                collective_id=0, has_side_effects=True, vmem_limit_bytes=40 * 1024 * 1024
            ),
        )(*(pltpu.with_memory_space_constraint(a, pltpu.HBM) for a in inputs))
        ready, scale, serve = pl.pallas_call(
            deliver,
            out_shape=outs,
            in_specs=[anywhere] * 3,
            out_specs=(anywhere,) * 3,
            scratch_shapes=[dma((experts + 2,))],
            compiler_params=pltpu.CompilerParams(vmem_limit_bytes=1024 * 1024),
        )(*results)
        return ready, scale, serve.T

    in_specs = (P("bank", None, "zero"), P("bank", None, "zero"), P("zero", "bank"), P("zero"))
    out_specs = (P("bank", "zero"), P("bank", "zero"), P())
    return jax.shard_map(local, mesh=mesh, in_specs=in_specs, out_specs=out_specs, check_vma=False)
```

```python
import functools

import jax
import jax.numpy as jnp
from jax import lax
from jax.experimental import pallas as pl
from jax.experimental.pallas import tpu as pltpu
from jax.sharding import PartitionSpec as P

MESH = pl.DeviceIdType.MESH
SUB, LANES = 8, 128
HALF = SUB // 2
PLANES = 4
CHUNKS = 8
UNIT = 40
SLABS = 2
DURING = 6


def remote(src, dst, send, recv, where):
    return pltpu.make_async_remote_copy(
        src_ref=src, dst_ref=dst, send_sem=send, recv_sem=recv, device_id=where, device_id_type=MESH
    )


def kernel(
    n, banks, train, other, weight, gain, ready, scale, serve,
    x_buf, o_buf, w_buf, g_buf, loose, part, heard, told, inv, sent, lines, raw_in,
    in_sem, max_send, max_recv, inv_send, inv_recv, row_send, row_recv, line_send, line_recv,
    send_sem, recv_sem, own_sem, raw_send, raw_recv,
):
    me, bank = lax.axis_index("zero"), lax.axis_index("bank")
    experts, _, rows, _ = x_buf.shape
    tiles, units = rows // SUB, rows // UNIT
    per, plane = n // CHUNKS, n // PLANES
    lane = lax.broadcasted_iota(jnp.int32, (SUB, LANES), 1)
    row = lax.broadcasted_iota(jnp.int32, (SUB, LANES), 0)

    def peer(up, i):
        z, x, c = lax.rem(me // plane + up, PLANES), lax.rem(me % plane // 2 + i // 2, plane // 2), lax.rem(me + i, 2)
        return z * plane + x * 2 + c

    planes = [lax.rem(me // plane + up, PLANES) * plane for up in range(PLANES)]
    places = [lax.rem(me % plane // 2 + i, plane // 2) * 2 for i in range(plane // 2)]
    cores = [lax.rem(me + i, 2) for i in range(2)]

    def back(up, i):
        z, x, c = lax.rem(me // plane + PLANES - up, PLANES), lax.rem(me % plane // 2 + plane // 2 - i // 2, plane // 2), lax.rem(me + i, 2)
        return z * plane + x * 2 + c

    half = lax.broadcasted_iota(jnp.int32, (HALF, LANES), 1)

    def packed(tile):
        return jnp.where(half < LANES // 2, tile[:HALF], pltpu.roll(tile[HALF:], LANES // 2, 1))

    def spread(tile):
        return jnp.concatenate([tile, pltpu.roll(tile, LANES // 2, 1)], axis=0)

    def others(body, ups=(2, 1, 3, 0)):
        for up in ups:
            for i in range(1 if up == 0 else 0, plane):
                body(planes[up] + places[i // 2] + cores[i % 2])

    def chunk(k):
        return lax.rem(me // plane * (plane // per) + plane // per + k, CHUNKS)

    def load(k):
        g = chunk(k)
        at = pl.ds(g * per, per)
        return (
            pltpu.make_async_copy(train.at[:, at], x_buf.at[:, at], in_sem.at[0, g]),
            pltpu.make_async_copy(other.at[:, at], o_buf.at[:, at], in_sem.at[1, g]),
        )

    small = (
        pltpu.make_async_copy(weight, w_buf, in_sem.at[0, CHUNKS]),
        pltpu.make_async_copy(gain, g_buf, in_sem.at[1, CHUNKS]),
    )
    barrier = pltpu.get_barrier_semaphore()
    for k in range(CHUNKS):
        for copy in load(k):
            copy.start()
    others(lambda d: pl.semaphore_signal(barrier, inc=1, device_id={"zero": d}, device_id_type=MESH))
    for copy in small:
        copy.start()

    across = lax.rem(bank + banks // 2, banks)
    row_of = banks // 2
    beside = [bank // row_of * row_of + lax.rem(bank + k, row_of) for k in range(1, row_of)]
    for b in [across] + beside:
        pl.semaphore_signal(barrier, inc=1, device_id={"bank": b}, device_id_type=MESH)

    def raw(way, u):
        slab, unit = u // units, u % units
        e, i = slab % experts, slab // experts
        d, at = peer(1 + 2 * way, i), pl.ds(unit * UNIT, UNIT)
        return remote(x_buf.at[e, d, at], raw_in.at[way, slab, at], raw_send.at[way, u], raw_recv.at[way, u], {"zero": d})

    def raws(first, last):
        for u in range(first, last):
            for way in range(2):
                raw(way, u).start()

    def maxima(k):
        for copy in load(k):
            copy.wait()
        for j in range(per):
            d = chunk(k) * per + j
            tile = jnp.zeros((SUB, LANES), jnp.float32)
            for e in range(experts):
                x = x_buf[e, d] + o_buf[e, d].astype(jnp.float32)
                x_buf[e, d] = x
                top = jnp.max(jnp.abs(x).reshape(tiles, SUB, LANES), axis=2, keepdims=True)
                for t in range(tiles):
                    tile = jnp.where(lane == e * tiles + t, top[t], tile)
            loose[j] = tile
        for j in range(per):
            part[chunk(k) * per + j] = packed(loose[j])

    def to_owner(d):
        return remote(part.at[d], heard.at[me], max_send.at[d], max_recv.at[me], {"zero": d})

    apart = CHUNKS - plane // per
    pl.loop(0, apart)(maxima)
    pl.semaphore_wait(barrier, n - 1 + row_of)
    others(lambda d: to_owner(d).start(), (2, 1, 3))
    pl.loop(apart, CHUNKS)(maxima)
    others(lambda d: to_owner(d).start(), (0,))

    raws(0, DURING)

    for copy in small:
        copy.wait()
    lines[bank, me] = (w_buf[...] * g_buf[...]).astype(jnp.bfloat16)

    def to_rows(d):
        return remote(lines.at[bank, me], lines.at[bank, me], row_send.at[d], row_recv.at[me], {"zero": d})

    def from_rows(s):
        remote(lines.at[bank, s], lines.at[bank, s], row_send.at[s], row_recv.at[s], {"zero": s}).wait_recv()

    def line(at, to, k):
        return remote(lines.at[at], lines.at[at], line_send.at[k], line_recv.at[k], {"bank": to})

    others(lambda d: to_rows(d).start())

    heard[me] = part[me]

    @pl.loop(0, n)
    def _(s):
        @pl.when(s != me)
        def _():
            remote(part.at[s], heard.at[s], max_send.at[s], max_recv.at[s], {"zero": s}).wait_recv()

    top = heard[0]
    for s in range(1, n):
        top = jnp.maximum(top, heard[s])
    used = lax.rem(half, LANES // 2) < experts * tiles
    told[0] = jnp.where(used, 1.0 / jnp.where(used, top, 1.0), 0.0)
    top = spread(top)

    def to_all(d):
        return remote(told.at[0], inv.at[me], inv_send.at[d], inv_recv.at[me], {"zero": d})

    others(lambda d: to_all(d).start(), (1, 3, 2, 0))

    raws(DURING, SLABS * units)

    def piece(e, at):
        return ready.at[e, :, pl.ds(pl.multiple_of(at * LANES, LANES), LANES)]

    def narrow(d, e, source, factor):
        factor = spread(factor)
        wide = [jnp.broadcast_to(factor[:, e * tiles + t : e * tiles + t + 1], (SUB, LANES)) for t in range(tiles)]
        sent[d, e] = (source * jnp.concatenate(wide, axis=0)).astype(jnp.bfloat16)

    def to_server(d, e):
        return remote(sent.at[d, e], piece(e, me), send_sem.at[d, e], recv_sem.at[me, e], {"zero": d})

    def known(d):
        remote(told.at[0], inv.at[d], inv_send.at[d], inv_recv.at[d], {"zero": d}).wait_recv()

    def step(up, i, was):
        d = peer(up, i)
        known(d)
        for e in range(experts):
            narrow(d, e, x_buf[e, d], inv[d])
        for e in range(experts):
            to_server(was, e).start()
        return d

    halves = [(peer(up, slab // experts), slab % experts) for slab in range(SLABS, -(-SLABS // experts) * experts) for up in (1, 3)]
    whole = -(-SLABS // experts)
    for d, e in halves:
        known(d)
        narrow(d, e, x_buf[e, d], inv[d])
    was = peer(1, whole)
    known(was)
    for e in range(experts):
        narrow(was, e, x_buf[e, was], inv[was])
    for d, e in halves:
        to_server(d, e).start()
    was = step(3, whole, was)

    @pl.loop(0, n)
    def _(s):
        @pl.when(s != me)
        def _():
            from_rows(s)

    line(bank, across, 0).start()

    was = lax.fori_loop(whole + 1, 4, lambda i, was: step(3, i, step(1, i, was)), was)

    was = lax.fori_loop(0, 4, lambda i, was: step(2, i, was), was)
    high = me // plane
    first = jnp.where(high == 0, 2, PLANES - high)
    second = jnp.where(high == 0, 1, jnp.where(high == 2, 3, 2))
    third = jnp.where(high == 1, 1, jnp.where(high == 2, 1, 3))
    was = lax.fori_loop(4, 6, lambda i, was: step(third, i, step(second, i, step(first, i, was))), was)
    was = lax.fori_loop(6, plane, lambda i, was: step(second, i, step(first, i, was)), was)
    was = lax.fori_loop(6, plane, lambda i, was: step(third, i, was), was)

    line(bank, across, 0).wait()
    for k, b in enumerate(beside):
        line(bank, b, 1 + k).start()
        line(across, b, row_of + k).start()

    was = lax.fori_loop(1, plane, lambda i, was: step(0, i, was), was)
    for e in range(experts):
        to_server(was, e).start()

    for e in range(experts):
        narrow(me, e, x_buf[e, me], told[0])
    local = [pltpu.make_async_copy(sent.at[me, e], piece(e, me), own_sem.at[e]) for e in range(experts)]
    for copy in local:
        copy.start()
    for slab in range(SLABS):
        e, i = slab % experts, slab // experts
        for way in range(2):
            slot, source = peer(1 + 2 * way, i), back(1 + 2 * way, i)
            for u in range(slab * units, slab * units + units):
                raw(way, u).wait()
            narrow(slot, e, raw_in[way, slab], told[0])
            local.append(pltpu.make_async_copy(sent.at[slot, e], piece(e, source), own_sem.at[experts + 2 * slab + way]))
            local[-1].start()

    for e in range(experts):
        for first in range(0, rows, LANES):
            width = min(LANES, rows - first)
            strip = jnp.zeros((SUB, LANES), jnp.float32)
            for t in range(first // SUB, (first + width) // SUB):
                c = e * tiles + t
                column = jnp.broadcast_to(top[:, c : c + 1], (SUB, LANES))
                strip = jnp.where(lane == t * SUB - first + row, column, strip)
            scale[e : e + 1, first : first + width] = jnp.max(strip, axis=0, keepdims=True)[:, :width]

    for copy in local:
        copy.wait()
    for k in range(1, row_of):
        b = bank // row_of * row_of + lax.rem(bank + row_of - k, row_of)
        far = lax.rem(b + banks // 2, banks)
        line(bank, beside[k - 1], k).wait_send()
        line(across, beside[k - 1], row_of + k - 1).wait_send()
        remote(lines.at[b], lines.at[b], line_send.at[k], line_recv.at[k], {"bank": b}).wait_recv()
        remote(lines.at[far], lines.at[far], line_send.at[row_of + k - 1], line_recv.at[row_of + k - 1], {"bank": b}).wait_recv()
    for s in range(n):
        columns = jnp.concatenate([lines[b, s].astype(jnp.float32) for b in range(banks)], axis=0)
        serve[:, s * LANES : (s + 1) * LANES] = columns.astype(jnp.bfloat16)

    @pl.loop(0, n)
    def _(d):
        @pl.when(d != me)
        def _():
            to_owner(d).wait_send()
            to_all(d).wait_send()
            to_rows(d).wait_send()

    for i in range(SLABS // experts):
        for up in (1, 3):
            known(peer(up, i))

    for slab in range(SLABS, whole * experts):
        for up in (1, 3):
            d, s, e = peer(up, slab // experts), back(up, slab // experts), slab % experts
            to_server(d, e).wait_send()
            remote(sent.at[s, e], piece(e, s), send_sem.at[s, e], recv_sem.at[s, e], {"zero": s}).wait_recv()

    def over(up, i):
        d, s = peer(up, i), back(up, i)
        for e in range(experts):
            to_server(d, e).wait_send()
            remote(sent.at[s, e], piece(e, s), send_sem.at[s, e], recv_sem.at[s, e], {"zero": s}).wait_recv()

    for lo, hi, ups in ((whole, 4, (1, 3)), (0, 4, (2,)), (4, plane, (1, 3, 2)), (1, plane, (0,))):

        @pl.loop(lo, hi)
        def _(i):
            for up in ups:
                over(up, i)


def deliver(ready, scale, serve, ready_out, scale_out, serve_out, sem):
    experts = ready.shape[0]
    copies = [pltpu.make_async_copy(ready.at[e], ready_out.at[e], sem.at[e]) for e in range(experts)]
    copies.append(pltpu.make_async_copy(scale, scale_out, sem.at[experts]))
    copies.append(pltpu.make_async_copy(serve, serve_out, sem.at[experts + 1]))
    for copy in copies:
        copy.start()
    for copy in copies:
        copy.wait()


def solution(mesh):
    n, banks = mesh.shape["zero"], mesh.shape["bank"]

    def local(train_down, other_down, router_weight, router_gain):
        experts, length, width = train_down.shape
        rows = length // n
        split = (experts, n, rows, width)
        dma, vmem = pltpu.SemaphoreType.DMA, pltpu.VMEM
        units = SLABS * rows // UNIT
        outs = (
            jax.ShapeDtypeStruct((experts, rows, n * width), jnp.bfloat16),
            jax.ShapeDtypeStruct((experts, rows), jnp.float32),
            jax.ShapeDtypeStruct((banks * experts, n * width), jnp.bfloat16),
        )
        anywhere = pl.BlockSpec(memory_space=pl.ANY)
        inputs = (train_down.reshape(split), other_down.reshape(split), router_weight.T, router_gain[None, :])
        results = pl.pallas_call(
            functools.partial(kernel, n, banks),
            out_shape=outs,
            in_specs=[pl.BlockSpec(memory_space=pltpu.HBM)] * 4,
            out_specs=(anywhere,) + (pl.BlockSpec(memory_space=vmem),) * 2,
            scratch_shapes=[
                vmem(split, jnp.float32),
                vmem(split, jnp.bfloat16),
                vmem((experts, width), jnp.float32),
                vmem((1, width), jnp.float32),
                vmem((n // CHUNKS, SUB, LANES), jnp.float32),
                vmem((n, HALF, LANES), jnp.float32),
                vmem((n, HALF, LANES), jnp.float32),
                vmem((1, HALF, LANES), jnp.float32),
                vmem((n, HALF, LANES), jnp.float32),
                vmem((n, experts, rows, width), jnp.bfloat16),
                vmem((banks, n, experts, width), jnp.bfloat16),
                vmem((2, SLABS, rows, width), jnp.float32),
                dma((2, CHUNKS + 1)),
                dma((n,)), dma((n,)), dma((n,)), dma((n,)),
                dma((n,)), dma((n,)), dma((banks,)), dma((banks,)),
                dma((n, experts)), dma((n, experts)), dma((experts + 2 * SLABS,)),
                dma((2, units)), dma((2, units)),
            ],
            compiler_params=pltpu.CompilerParams(
                collective_id=0, has_side_effects=True, vmem_limit_bytes=40 * 1024 * 1024
            ),
        )(*(pltpu.with_memory_space_constraint(a, pltpu.HBM) for a in inputs))
        ready, scale, serve = pl.pallas_call(
            deliver,
            out_shape=outs,
            in_specs=[anywhere] * 3,
            out_specs=(anywhere,) * 3,
            scratch_shapes=[dma((experts + 2,))],
            compiler_params=pltpu.CompilerParams(vmem_limit_bytes=1024 * 1024),
        )(*results)
        return ready, scale, serve.T

    in_specs = (P("bank", None, "zero"), P("bank", None, "zero"), P("zero", "bank"), P("zero"))
    out_specs = (P("bank", "zero"), P("bank", "zero"), P())
    return jax.shard_map(local, mesh=mesh, in_specs=in_specs, out_specs=out_specs, check_vma=False)
```

```python
import functools

import jax
import jax.numpy as jnp
from jax import lax
from jax.experimental import pallas as pl
from jax.experimental.pallas import tpu as pltpu
from jax.sharding import PartitionSpec as P

MESH = pl.DeviceIdType.MESH
SUB, LANES = 8, 128
HALF = SUB // 2
PLANES = 4
CHUNKS = 8
UNIT = 200
SLABS = 2
DURING = 1


def remote(src, dst, send, recv, where):
    return pltpu.make_async_remote_copy(
        src_ref=src, dst_ref=dst, send_sem=send, recv_sem=recv, device_id=where, device_id_type=MESH
    )


def kernel(
    n, banks, train, other, weight, gain, ready, scale, serve,
    x_buf, o_buf, w_buf, g_buf, loose, part, heard, told, inv, sent, lines, raw_in,
    in_sem, max_send, max_recv, inv_send, inv_recv, row_send, row_recv, line_send, line_recv,
    send_sem, recv_sem, own_sem, raw_send, raw_recv,
):
    me, bank = lax.axis_index("zero"), lax.axis_index("bank")
    experts, _, rows, _ = x_buf.shape
    tiles, units = rows // SUB, rows // UNIT
    per, plane = n // CHUNKS, n // PLANES
    lane = lax.broadcasted_iota(jnp.int32, (SUB, LANES), 1)
    row = lax.broadcasted_iota(jnp.int32, (SUB, LANES), 0)

    def peer(up, i):
        z, x, c = lax.rem(me // plane + up, PLANES), lax.rem(me % plane // 2 + i // 2, plane // 2), lax.rem(me + i, 2)
        return z * plane + x * 2 + c

    planes = [lax.rem(me // plane + up, PLANES) * plane for up in range(PLANES)]
    places = [lax.rem(me % plane // 2 + i, plane // 2) * 2 for i in range(plane // 2)]
    cores = [lax.rem(me + i, 2) for i in range(2)]

    def back(up, i):
        z, x, c = lax.rem(me // plane + PLANES - up, PLANES), lax.rem(me % plane // 2 + plane // 2 - i // 2, plane // 2), lax.rem(me + i, 2)
        return z * plane + x * 2 + c

    half = lax.broadcasted_iota(jnp.int32, (HALF, LANES), 1)

    def packed(tile):
        return jnp.where(half < LANES // 2, tile[:HALF], pltpu.roll(tile[HALF:], LANES // 2, 1))

    def spread(tile):
        return jnp.concatenate([tile, pltpu.roll(tile, LANES // 2, 1)], axis=0)

    def others(body, ups=(2, 1, 3, 0)):
        for up in ups:
            for i in range(1 if up == 0 else 0, plane):
                body(planes[up] + places[i // 2] + cores[i % 2])

    def chunk(k):
        return lax.rem(me // plane * (plane // per) + plane // per + k, CHUNKS)

    def load(k):
        g = chunk(k)
        at = pl.ds(g * per, per)
        return (
            pltpu.make_async_copy(train.at[:, at], x_buf.at[:, at], in_sem.at[0, g]),
            pltpu.make_async_copy(other.at[:, at], o_buf.at[:, at], in_sem.at[1, g]),
        )

    small = (
        pltpu.make_async_copy(weight, w_buf, in_sem.at[0, CHUNKS]),
        pltpu.make_async_copy(gain, g_buf, in_sem.at[1, CHUNKS]),
    )
    barrier = pltpu.get_barrier_semaphore()
    for k in range(CHUNKS):
        for copy in load(k):
            copy.start()
    others(lambda d: pl.semaphore_signal(barrier, inc=1, device_id={"zero": d}, device_id_type=MESH))
    for copy in small:
        copy.start()

    across = lax.rem(bank + banks // 2, banks)
    row_of = banks // 2
    beside = [bank // row_of * row_of + lax.rem(bank + k, row_of) for k in range(1, row_of)]
    for b in [across] + beside:
        pl.semaphore_signal(barrier, inc=1, device_id={"bank": b}, device_id_type=MESH)

    def raw(way, u):
        slab, unit = u // units, u % units
        e, i = slab % experts, slab // experts
        d, at = peer(1 + 2 * way, i), pl.ds(unit * UNIT, UNIT)
        return remote(x_buf.at[e, d, at], raw_in.at[way, slab, at], raw_send.at[way, u], raw_recv.at[way, u], {"zero": d})

    def raws(first, last):
        for u in range(first, last):
            for way in range(2):
                raw(way, u).start()

    def maxima(k):
        for copy in load(k):
            copy.wait()
        for j in range(per):
            d = chunk(k) * per + j
            tile = jnp.zeros((SUB, LANES), jnp.float32)
            for e in range(experts):
                x = x_buf[e, d] + o_buf[e, d].astype(jnp.float32)
                x_buf[e, d] = x
                top = jnp.max(jnp.abs(x).reshape(tiles, SUB, LANES), axis=2, keepdims=True)
                for t in range(tiles):
                    tile = jnp.where(lane == e * tiles + t, top[t], tile)
            loose[j] = tile
        for j in range(per):
            part[chunk(k) * per + j] = packed(loose[j])

    def to_owner(d):
        return remote(part.at[d], heard.at[me], max_send.at[d], max_recv.at[me], {"zero": d})

    apart = CHUNKS - plane // per
    pl.loop(0, apart)(maxima)
    pl.semaphore_wait(barrier, n - 1 + row_of)
    others(lambda d: to_owner(d).start(), (2, 1, 3))
    pl.loop(apart, CHUNKS)(maxima)
    others(lambda d: to_owner(d).start(), (0,))

    raws(0, DURING)

    for copy in small:
        copy.wait()
    lines[bank, me] = (w_buf[...] * g_buf[...]).astype(jnp.bfloat16)

    def to_rows(d):
        return remote(lines.at[bank, me], lines.at[bank, me], row_send.at[d], row_recv.at[me], {"zero": d})

    def from_rows(s):
        remote(lines.at[bank, s], lines.at[bank, s], row_send.at[s], row_recv.at[s], {"zero": s}).wait_recv()

    def line(at, to, k):
        return remote(lines.at[at], lines.at[at], line_send.at[k], line_recv.at[k], {"bank": to})

    others(lambda d: to_rows(d).start())

    heard[me] = part[me]

    @pl.loop(0, n)
    def _(s):
        @pl.when(s != me)
        def _():
            remote(part.at[s], heard.at[s], max_send.at[s], max_recv.at[s], {"zero": s}).wait_recv()

    top = heard[0]
    for s in range(1, n):
        top = jnp.maximum(top, heard[s])
    used = lax.rem(half, LANES // 2) < experts * tiles
    told[0] = jnp.where(used, 1.0 / jnp.where(used, top, 1.0), 0.0)
    top = spread(top)

    def to_all(d):
        return remote(told.at[0], inv.at[me], inv_send.at[d], inv_recv.at[me], {"zero": d})

    others(lambda d: to_all(d).start(), (1, 3, 0, 2))

    raws(DURING, SLABS * units)

    def piece(e, at):
        return ready.at[e, :, pl.ds(pl.multiple_of(at * LANES, LANES), LANES)]

    def narrow(d, e, source, factor):
        factor = spread(factor)
        wide = [jnp.broadcast_to(factor[:, e * tiles + t : e * tiles + t + 1], (SUB, LANES)) for t in range(tiles)]
        sent[d, e] = (source * jnp.concatenate(wide, axis=0)).astype(jnp.bfloat16)

    def to_server(d, e):
        return remote(sent.at[d, e], piece(e, me), send_sem.at[d, e], recv_sem.at[me, e], {"zero": d})

    def known(d):
        remote(told.at[0], inv.at[d], inv_send.at[d], inv_recv.at[d], {"zero": d}).wait_recv()

    def step(up, i, was):
        d = peer(up, i)
        known(d)
        for e in range(experts):
            narrow(d, e, x_buf[e, d], inv[d])
        for e in range(experts):
            to_server(was, e).start()
        return d

    halves = [(peer(up, slab // experts), slab % experts) for slab in range(SLABS, -(-SLABS // experts) * experts) for up in (1, 3)]
    whole = -(-SLABS // experts)
    for d, e in halves:
        known(d)
        narrow(d, e, x_buf[e, d], inv[d])
    was = peer(1, whole)
    known(was)
    for e in range(experts):
        narrow(was, e, x_buf[e, was], inv[was])
    for d, e in halves:
        to_server(d, e).start()
    was = step(3, whole, was)

    @pl.loop(0, n)
    def _(s):
        @pl.when(s != me)
        def _():
            from_rows(s)

    line(bank, across, 0).start()

    was = lax.fori_loop(whole + 1, 4, lambda i, was: step(3, i, step(1, i, was)), was)

    was = lax.fori_loop(0, 4, lambda i, was: step(2, i, was), was)
    was = lax.fori_loop(1, 4, lambda i, was: step(0, i, was), was)
    high = me // plane
    first = jnp.where(high == 0, 2, PLANES - high)
    second = jnp.where(high == 0, 1, jnp.where(high == 2, 3, 2))
    third = jnp.where(high == 1, 1, jnp.where(high == 2, 1, 3))
    was = lax.fori_loop(4, 6, lambda i, was: step(third, i, step(second, i, step(first, i, was))), was)
    was = lax.fori_loop(6, plane, lambda i, was: step(second, i, step(first, i, was)), was)
    was = lax.fori_loop(6, plane, lambda i, was: step(third, i, was), was)

    was = lax.fori_loop(4, plane, lambda i, was: step(0, i, was), was)

    line(bank, across, 0).wait()
    for k, b in enumerate(beside):
        line(bank, b, 1 + k).start()
        line(across, b, row_of + k).start()

    for e in range(experts):
        to_server(was, e).start()

    for e in range(experts):
        narrow(me, e, x_buf[e, me], told[0])
    local = [pltpu.make_async_copy(sent.at[me, e], piece(e, me), own_sem.at[e]) for e in range(experts)]
    for copy in local:
        copy.start()
    for slab in range(SLABS):
        e, i = slab % experts, slab // experts
        for way in range(2):
            slot, source = peer(1 + 2 * way, i), back(1 + 2 * way, i)
            for u in range(slab * units, slab * units + units):
                raw(way, u).wait()
            narrow(slot, e, raw_in[way, slab], told[0])
            local.append(pltpu.make_async_copy(sent.at[slot, e], piece(e, source), own_sem.at[experts + 2 * slab + way]))
            local[-1].start()

    for e in range(experts):
        for first in range(0, rows, LANES):
            width = min(LANES, rows - first)
            strip = jnp.zeros((SUB, LANES), jnp.float32)
            for t in range(first // SUB, (first + width) // SUB):
                c = e * tiles + t
                column = jnp.broadcast_to(top[:, c : c + 1], (SUB, LANES))
                strip = jnp.where(lane == t * SUB - first + row, column, strip)
            scale[e : e + 1, first : first + width] = jnp.max(strip, axis=0, keepdims=True)[:, :width]

    for copy in local:
        copy.wait()
    for k in range(1, row_of):
        b = bank // row_of * row_of + lax.rem(bank + row_of - k, row_of)
        far = lax.rem(b + banks // 2, banks)
        line(bank, beside[k - 1], k).wait_send()
        line(across, beside[k - 1], row_of + k - 1).wait_send()
        remote(lines.at[b], lines.at[b], line_send.at[k], line_recv.at[k], {"bank": b}).wait_recv()
        remote(lines.at[far], lines.at[far], line_send.at[row_of + k - 1], line_recv.at[row_of + k - 1], {"bank": b}).wait_recv()
    for s in range(n):
        columns = jnp.concatenate([lines[b, s].astype(jnp.float32) for b in range(banks)], axis=0)
        serve[:, s * LANES : (s + 1) * LANES] = columns.astype(jnp.bfloat16)

    @pl.loop(0, n)
    def _(d):
        @pl.when(d != me)
        def _():
            to_owner(d).wait_send()
            to_all(d).wait_send()
            to_rows(d).wait_send()

    for i in range(SLABS // experts):
        for up in (1, 3):
            known(peer(up, i))

    for slab in range(SLABS, whole * experts):
        for up in (1, 3):
            d, s, e = peer(up, slab // experts), back(up, slab // experts), slab % experts
            to_server(d, e).wait_send()
            remote(sent.at[s, e], piece(e, s), send_sem.at[s, e], recv_sem.at[s, e], {"zero": s}).wait_recv()

    def over(up, i):
        d, s = peer(up, i), back(up, i)
        for e in range(experts):
            to_server(d, e).wait_send()
            remote(sent.at[s, e], piece(e, s), send_sem.at[s, e], recv_sem.at[s, e], {"zero": s}).wait_recv()

    for lo, hi, ups in ((whole, 4, (1, 3)), (0, 4, (2,)), (4, plane, (1, 3, 2)), (1, plane, (0,))):

        @pl.loop(lo, hi)
        def _(i):
            for up in ups:
                over(up, i)


def deliver(ready, scale, serve, ready_out, scale_out, serve_out, sem):
    experts = ready.shape[0]
    copies = [pltpu.make_async_copy(ready.at[e], ready_out.at[e], sem.at[e]) for e in range(experts)]
    copies.append(pltpu.make_async_copy(scale, scale_out, sem.at[experts]))
    copies.append(pltpu.make_async_copy(serve, serve_out, sem.at[experts + 1]))
    for copy in copies:
        copy.start()
    for copy in copies:
        copy.wait()


def solution(mesh):
    n, banks = mesh.shape["zero"], mesh.shape["bank"]

    def local(train_down, other_down, router_weight, router_gain):
        experts, length, width = train_down.shape
        rows = length // n
        split = (experts, n, rows, width)
        dma, vmem = pltpu.SemaphoreType.DMA, pltpu.VMEM
        units = SLABS * rows // UNIT
        outs = (
            jax.ShapeDtypeStruct((experts, rows, n * width), jnp.bfloat16),
            jax.ShapeDtypeStruct((experts, rows), jnp.float32),
            jax.ShapeDtypeStruct((banks * experts, n * width), jnp.bfloat16),
        )
        anywhere = pl.BlockSpec(memory_space=pl.ANY)
        inputs = (train_down.reshape(split), other_down.reshape(split), router_weight.T, router_gain[None, :])
        results = pl.pallas_call(
            functools.partial(kernel, n, banks),
            out_shape=outs,
            in_specs=[pl.BlockSpec(memory_space=pltpu.HBM)] * 4,
            out_specs=(anywhere,) + (pl.BlockSpec(memory_space=vmem),) * 2,
            scratch_shapes=[
                vmem(split, jnp.float32),
                vmem(split, jnp.bfloat16),
                vmem((experts, width), jnp.float32),
                vmem((1, width), jnp.float32),
                vmem((n // CHUNKS, SUB, LANES), jnp.float32),
                vmem((n, HALF, LANES), jnp.float32),
                vmem((n, HALF, LANES), jnp.float32),
                vmem((1, HALF, LANES), jnp.float32),
                vmem((n, HALF, LANES), jnp.float32),
                vmem((n, experts, rows, width), jnp.bfloat16),
                vmem((banks, n, experts, width), jnp.bfloat16),
                vmem((2, SLABS, rows, width), jnp.float32),
                dma((2, CHUNKS + 1)),
                dma((n,)), dma((n,)), dma((n,)), dma((n,)),
                dma((n,)), dma((n,)), dma((banks,)), dma((banks,)),
                dma((n, experts)), dma((n, experts)), dma((experts + 2 * SLABS,)),
                dma((2, units)), dma((2, units)),
            ],
            compiler_params=pltpu.CompilerParams(
                collective_id=0, has_side_effects=True, vmem_limit_bytes=40 * 1024 * 1024
            ),
        )(*(pltpu.with_memory_space_constraint(a, pltpu.HBM) for a in inputs))
        ready, scale, serve = pl.pallas_call(
            deliver,
            out_shape=outs,
            in_specs=[anywhere] * 3,
            out_specs=(anywhere,) * 3,
            scratch_shapes=[dma((experts + 2,))],
            compiler_params=pltpu.CompilerParams(vmem_limit_bytes=1024 * 1024),
        )(*results)
        return ready, scale, serve.T

    in_specs = (P("bank", None, "zero"), P("bank", None, "zero"), P("zero", "bank"), P("zero"))
    out_specs = (P("bank", "zero"), P("bank", "zero"), P())
    return jax.shard_map(local, mesh=mesh, in_specs=in_specs, out_specs=out_specs, check_vma=False)
```

```python
import functools

import jax
import jax.numpy as jnp
from jax import lax
from jax.experimental import pallas as pl
from jax.experimental.pallas import tpu as pltpu
from jax.sharding import PartitionSpec as P

MESH = pl.DeviceIdType.MESH
SUB, LANES = 8, 128
HALF = SUB // 2
PLANES = 4
CHUNKS = 8
UNIT = 200
SLABS = 2
DURING = 1


def remote(src, dst, send, recv, where):
    return pltpu.make_async_remote_copy(
        src_ref=src, dst_ref=dst, send_sem=send, recv_sem=recv, device_id=where, device_id_type=MESH
    )


def kernel(
    n, banks, train, other, weight, gain, ready, scale, serve,
    x_buf, o_buf, w_buf, g_buf, loose, part, heard, told, inv, sent, lines, raw_in,
    in_sem, max_send, max_recv, inv_send, inv_recv, row_send, row_recv, line_send, line_recv,
    send_sem, recv_sem, own_sem, raw_send, raw_recv,
):
    me, bank = lax.axis_index("zero"), lax.axis_index("bank")
    experts, _, rows, _ = x_buf.shape
    tiles, units = rows // SUB, rows // UNIT
    per, plane = n // CHUNKS, n // PLANES
    lane = lax.broadcasted_iota(jnp.int32, (SUB, LANES), 1)
    row = lax.broadcasted_iota(jnp.int32, (SUB, LANES), 0)

    def peer(up, i):
        z, x, c = lax.rem(me // plane + up, PLANES), lax.rem(me % plane // 2 + i // 2, plane // 2), lax.rem(me + i, 2)
        return z * plane + x * 2 + c

    planes = [lax.rem(me // plane + up, PLANES) * plane for up in range(PLANES)]
    places = [lax.rem(me % plane // 2 + i, plane // 2) * 2 for i in range(plane // 2)]
    cores = [lax.rem(me + i, 2) for i in range(2)]

    def back(up, i):
        z, x, c = lax.rem(me // plane + PLANES - up, PLANES), lax.rem(me % plane // 2 + plane // 2 - i // 2, plane // 2), lax.rem(me + i, 2)
        return z * plane + x * 2 + c

    half = lax.broadcasted_iota(jnp.int32, (HALF, LANES), 1)

    def packed(tile):
        return jnp.where(half < LANES // 2, tile[:HALF], pltpu.roll(tile[HALF:], LANES // 2, 1))

    def spread(tile):
        return jnp.concatenate([tile, pltpu.roll(tile, LANES // 2, 1)], axis=0)

    def others(body, ups=(2, 1, 3, 0)):
        for up in ups:
            for i in range(1 if up == 0 else 0, plane):
                body(planes[up] + places[i // 2] + cores[i % 2])

    def chunk(k):
        return lax.rem(me // plane * (plane // per) + plane // per + k, CHUNKS)

    def load(k):
        g = chunk(k)
        at = pl.ds(g * per, per)
        return (
            pltpu.make_async_copy(train.at[:, at], x_buf.at[:, at], in_sem.at[0, g]),
            pltpu.make_async_copy(other.at[:, at], o_buf.at[:, at], in_sem.at[1, g]),
        )

    small = (
        pltpu.make_async_copy(weight, w_buf, in_sem.at[0, CHUNKS]),
        pltpu.make_async_copy(gain, g_buf, in_sem.at[1, CHUNKS]),
    )
    barrier = pltpu.get_barrier_semaphore()
    for k in range(CHUNKS):
        for copy in load(k):
            copy.start()
    others(lambda d: pl.semaphore_signal(barrier, inc=1, device_id={"zero": d}, device_id_type=MESH))
    for copy in small:
        copy.start()

    across = lax.rem(bank + banks // 2, banks)
    row_of = banks // 2
    beside = [bank // row_of * row_of + lax.rem(bank + k, row_of) for k in range(1, row_of)]
    for b in [across] + beside:
        pl.semaphore_signal(barrier, inc=1, device_id={"bank": b}, device_id_type=MESH)

    def raw(way, u):
        slab, unit = u // units, u % units
        e, i = slab % experts, slab // experts
        d, at = peer(1 + 2 * way, i), pl.ds(unit * UNIT, UNIT)
        return remote(x_buf.at[e, d, at], raw_in.at[way, slab, at], raw_send.at[way, u], raw_recv.at[way, u], {"zero": d})

    def raws(first, last):
        for u in range(first, last):
            for way in range(2):
                raw(way, u).start()

    def maxima(k):
        for copy in load(k):
            copy.wait()
        for j in range(per):
            d = chunk(k) * per + j
            tile = jnp.zeros((SUB, LANES), jnp.float32)
            for e in range(experts):
                x = x_buf[e, d] + o_buf[e, d].astype(jnp.float32)
                x_buf[e, d] = x
                top = jnp.max(jnp.abs(x).reshape(tiles, SUB, LANES), axis=2, keepdims=True)
                for t in range(tiles):
                    tile = jnp.where(lane == e * tiles + t, top[t], tile)
            loose[j] = tile
        for j in range(per):
            part[chunk(k) * per + j] = packed(loose[j])

    def to_owner(d):
        return remote(part.at[d], heard.at[me], max_send.at[d], max_recv.at[me], {"zero": d})

    apart = CHUNKS - plane // per
    pl.loop(0, apart)(maxima)
    pl.semaphore_wait(barrier, n - 1 + row_of)
    others(lambda d: to_owner(d).start(), (2, 1, 3))
    pl.loop(apart, CHUNKS)(maxima)
    others(lambda d: to_owner(d).start(), (0,))

    raws(0, DURING)

    for copy in small:
        copy.wait()
    lines[bank, me] = (w_buf[...] * g_buf[...]).astype(jnp.bfloat16)

    def to_rows(d):
        return remote(lines.at[bank, me], lines.at[bank, me], row_send.at[d], row_recv.at[me], {"zero": d})

    def from_rows(s):
        remote(lines.at[bank, s], lines.at[bank, s], row_send.at[s], row_recv.at[s], {"zero": s}).wait_recv()

    def line(at, to, k):
        return remote(lines.at[at], lines.at[at], line_send.at[k], line_recv.at[k], {"bank": to})

    others(lambda d: to_rows(d).start())

    heard[me] = part[me]

    @pl.loop(0, n)
    def _(s):
        @pl.when(s != me)
        def _():
            remote(part.at[s], heard.at[s], max_send.at[s], max_recv.at[s], {"zero": s}).wait_recv()

    top = heard[0]
    for s in range(1, n):
        top = jnp.maximum(top, heard[s])
    used = lax.rem(half, LANES // 2) < experts * tiles
    told[0] = jnp.where(used, 1.0 / jnp.where(used, top, 1.0), 0.0)
    top = spread(top)

    def to_all(d):
        return remote(told.at[0], inv.at[me], inv_send.at[d], inv_recv.at[me], {"zero": d})

    others(lambda d: to_all(d).start(), (1, 3, 0, 2))

    raws(DURING, SLABS * units)

    def piece(e, at):
        return ready.at[e, :, pl.ds(pl.multiple_of(at * LANES, LANES), LANES)]

    def narrow(d, e, source, factor):
        factor = spread(factor)
        wide = [jnp.broadcast_to(factor[:, e * tiles + t : e * tiles + t + 1], (SUB, LANES)) for t in range(tiles)]
        sent[d, e] = (source * jnp.concatenate(wide, axis=0)).astype(jnp.bfloat16)

    def to_server(d, e):
        return remote(sent.at[d, e], piece(e, me), send_sem.at[d, e], recv_sem.at[me, e], {"zero": d})

    def known(d):
        remote(told.at[0], inv.at[d], inv_send.at[d], inv_recv.at[d], {"zero": d}).wait_recv()

    def step(up, i, was):
        d = peer(up, i)
        known(d)
        for e in range(experts):
            narrow(d, e, x_buf[e, d], inv[d])
        for e in range(experts):
            to_server(was, e).start()
        return d

    halves = [(peer(up, slab // experts), slab % experts) for slab in range(SLABS, -(-SLABS // experts) * experts) for up in (1, 3)]
    whole = -(-SLABS // experts)
    for d, e in halves:
        known(d)
        narrow(d, e, x_buf[e, d], inv[d])
    was = peer(1, whole)
    known(was)
    for e in range(experts):
        narrow(was, e, x_buf[e, was], inv[was])
    for d, e in halves:
        to_server(d, e).start()
    was = step(3, whole, was)

    @pl.loop(0, n)
    def _(s):
        @pl.when(s != me)
        def _():
            from_rows(s)

    line(bank, across, 0).start()

    was = lax.fori_loop(whole + 1, 4, lambda i, was: step(3, i, step(1, i, was)), was)

    was = lax.fori_loop(0, 4, lambda i, was: step(2, i, was), was)
    was = lax.fori_loop(1, 4, lambda i, was: step(0, i, was), was)
    high = me // plane
    first = jnp.where(high == 0, 2, PLANES - high)
    second = jnp.where(high == 0, 1, jnp.where(high == 2, 3, 2))
    third = jnp.where(high == 1, 1, jnp.where(high == 2, 1, 3))
    was = lax.fori_loop(4, 6, lambda i, was: step(third, i, step(second, i, step(first, i, was))), was)
    was = lax.fori_loop(6, plane, lambda i, was: step(first, i, was), was)
    was = lax.fori_loop(6, plane, lambda i, was: step(third, i, step(second, i, was)), was)

    was = lax.fori_loop(4, plane, lambda i, was: step(0, i, was), was)

    line(bank, across, 0).wait()
    for k, b in enumerate(beside):
        line(bank, b, 1 + k).start()
        line(across, b, row_of + k).start()

    for e in range(experts):
        to_server(was, e).start()

    for e in range(experts):
        narrow(me, e, x_buf[e, me], told[0])
    local = [pltpu.make_async_copy(sent.at[me, e], piece(e, me), own_sem.at[e]) for e in range(experts)]
    for copy in local:
        copy.start()
    for slab in range(SLABS):
        e, i = slab % experts, slab // experts
        for way in range(2):
            slot, source = peer(1 + 2 * way, i), back(1 + 2 * way, i)
            for u in range(slab * units, slab * units + units):
                raw(way, u).wait()
            narrow(slot, e, raw_in[way, slab], told[0])
            local.append(pltpu.make_async_copy(sent.at[slot, e], piece(e, source), own_sem.at[experts + 2 * slab + way]))
            local[-1].start()

    for e in range(experts):
        for first in range(0, rows, LANES):
            width = min(LANES, rows - first)
            strip = jnp.zeros((SUB, LANES), jnp.float32)
            for t in range(first // SUB, (first + width) // SUB):
                c = e * tiles + t
                column = jnp.broadcast_to(top[:, c : c + 1], (SUB, LANES))
                strip = jnp.where(lane == t * SUB - first + row, column, strip)
            scale[e : e + 1, first : first + width] = jnp.max(strip, axis=0, keepdims=True)[:, :width]

    for copy in local:
        copy.wait()
    for k in range(1, row_of):
        b = bank // row_of * row_of + lax.rem(bank + row_of - k, row_of)
        far = lax.rem(b + banks // 2, banks)
        line(bank, beside[k - 1], k).wait_send()
        line(across, beside[k - 1], row_of + k - 1).wait_send()
        remote(lines.at[b], lines.at[b], line_send.at[k], line_recv.at[k], {"bank": b}).wait_recv()
        remote(lines.at[far], lines.at[far], line_send.at[row_of + k - 1], line_recv.at[row_of + k - 1], {"bank": b}).wait_recv()
    for s in range(n):
        columns = jnp.concatenate([lines[b, s].astype(jnp.float32) for b in range(banks)], axis=0)
        serve[:, s * LANES : (s + 1) * LANES] = columns.astype(jnp.bfloat16)

    @pl.loop(0, n)
    def _(d):
        @pl.when(d != me)
        def _():
            to_owner(d).wait_send()
            to_all(d).wait_send()
            to_rows(d).wait_send()

    for i in range(SLABS // experts):
        for up in (1, 3):
            known(peer(up, i))

    for slab in range(SLABS, whole * experts):
        for up in (1, 3):
            d, s, e = peer(up, slab // experts), back(up, slab // experts), slab % experts
            to_server(d, e).wait_send()
            remote(sent.at[s, e], piece(e, s), send_sem.at[s, e], recv_sem.at[s, e], {"zero": s}).wait_recv()

    def over(up, i):
        d, s = peer(up, i), back(up, i)
        for e in range(experts):
            to_server(d, e).wait_send()
            remote(sent.at[s, e], piece(e, s), send_sem.at[s, e], recv_sem.at[s, e], {"zero": s}).wait_recv()

    for lo, hi, ups in ((whole, 4, (1, 3)), (0, 4, (2,)), (4, plane, (1, 3, 2)), (1, plane, (0,))):

        @pl.loop(lo, hi)
        def _(i):
            for up in ups:
                over(up, i)


def deliver(ready, scale, serve, ready_out, scale_out, serve_out, sem):
    experts = ready.shape[0]
    copies = [pltpu.make_async_copy(ready.at[e], ready_out.at[e], sem.at[e]) for e in range(experts)]
    copies.append(pltpu.make_async_copy(scale, scale_out, sem.at[experts]))
    copies.append(pltpu.make_async_copy(serve, serve_out, sem.at[experts + 1]))
    for copy in copies:
        copy.start()
    for copy in copies:
        copy.wait()


def solution(mesh):
    n, banks = mesh.shape["zero"], mesh.shape["bank"]

    def local(train_down, other_down, router_weight, router_gain):
        experts, length, width = train_down.shape
        rows = length // n
        split = (experts, n, rows, width)
        dma, vmem = pltpu.SemaphoreType.DMA, pltpu.VMEM
        units = SLABS * rows // UNIT
        outs = (
            jax.ShapeDtypeStruct((experts, rows, n * width), jnp.bfloat16),
            jax.ShapeDtypeStruct((experts, rows), jnp.float32),
            jax.ShapeDtypeStruct((banks * experts, n * width), jnp.bfloat16),
        )
        anywhere = pl.BlockSpec(memory_space=pl.ANY)
        inputs = (train_down.reshape(split), other_down.reshape(split), router_weight.T, router_gain[None, :])
        results = pl.pallas_call(
            functools.partial(kernel, n, banks),
            out_shape=outs,
            in_specs=[pl.BlockSpec(memory_space=pltpu.HBM)] * 4,
            out_specs=(anywhere,) + (pl.BlockSpec(memory_space=vmem),) * 2,
            scratch_shapes=[
                vmem(split, jnp.float32),
                vmem(split, jnp.bfloat16),
                vmem((experts, width), jnp.float32),
                vmem((1, width), jnp.float32),
                vmem((n // CHUNKS, SUB, LANES), jnp.float32),
                vmem((n, HALF, LANES), jnp.float32),
                vmem((n, HALF, LANES), jnp.float32),
                vmem((1, HALF, LANES), jnp.float32),
                vmem((n, HALF, LANES), jnp.float32),
                vmem((n, experts, rows, width), jnp.bfloat16),
                vmem((banks, n, experts, width), jnp.bfloat16),
                vmem((2, SLABS, rows, width), jnp.float32),
                dma((2, CHUNKS + 1)),
                dma((n,)), dma((n,)), dma((n,)), dma((n,)),
                dma((n,)), dma((n,)), dma((banks,)), dma((banks,)),
                dma((n, experts)), dma((n, experts)), dma((experts + 2 * SLABS,)),
                dma((2, units)), dma((2, units)),
            ],
            compiler_params=pltpu.CompilerParams(
                collective_id=0, has_side_effects=True, vmem_limit_bytes=40 * 1024 * 1024
            ),
        )(*(pltpu.with_memory_space_constraint(a, pltpu.HBM) for a in inputs))
        ready, scale, serve = pl.pallas_call(
            deliver,
            out_shape=outs,
            in_specs=[anywhere] * 3,
            out_specs=(anywhere,) * 3,
            scratch_shapes=[dma((experts + 2,))],
            compiler_params=pltpu.CompilerParams(vmem_limit_bytes=1024 * 1024),
        )(*results)
        return ready, scale, serve.T

    in_specs = (P("bank", None, "zero"), P("bank", None, "zero"), P("zero", "bank"), P("zero"))
    out_specs = (P("bank", "zero"), P("bank", "zero"), P())
    return jax.shard_map(local, mesh=mesh, in_specs=in_specs, out_specs=out_specs, check_vma=False)
```
